128 devices in a mesh: gz: 2 (over x_lo), gx: 2 (over core), gy: 32 (over z, y, x_hi).
Axes of the slice: x: 4 (x_hi: 2, x_lo: 2; x = x_hi * 2 + x_lo), y: 4, z: 4, core: 2. Of those that a mesh axis runs over, the one named last changes fastest.
Arguments:
- initial_field: float32 [128, 16, 4096], P('gz', 'gx', 'gy'), may hold values from -36 to 36
- plane_coupling: float32 [128, 16, 4096], P('gz', 'gx', 'gy'), may hold values from 0.06 to 0.24
- line_coupling: float32 [128, 16, 4096], P('gz', 'gx', 'gy'), may hold values from 1000 to 8000
- source: float32 [128, 16, 4096], P('gz', 'gx', 'gy'), may hold values from -4 to 4, as said below
- shift_table: float32 [8], replicated, may hold values from 0.5 to 1
- shift_index: int32 [4], replicated, may hold values from 0 to 7
Outputs:
- heated: float32 [128, 16, 4096], P('gz', 'gx', 'gy')
The draws below stay inside these ranges and needn't reach their ends.
Inputs may be any that keep to these rules, and one draw needn't show every extreme that they name: `shift_index`: one table row for each half-step. A heat source.
All inputs are finite; a program needn't handle non-finite values.
Results may differ from the reference program's by a relative error of at most 0.0003.
Values sent between devices are 32-bit elements; how exact they have to be, the bound alone decides.
A program may use at most 64 MiB of HBM per device.

```python
import math
import jax
import jax.numpy as jnp
from jax import lax

SHIFTS = 8
HALF = 4
NX = 16
NY = 4096
NZ = 128


def draw_source(key, part):
    values = jnp.clip(jax.random.normal(key, (NZ, NX, NY), jnp.float32), -4.0, 4.0)
    return values


def place_ends(entries, rng, least, top_value):
    dims = entries.shape
    place = [jax.random.randint(jax.random.fold_in(rng, axis), (), 0, dims[axis]) for axis in range(len(dims))]
    entries = entries.at[tuple(place)].set(least)
    longest = dims.index(max(dims))
    place[longest] = (place[longest] + 1) % dims[longest]
    return entries.at[tuple(place)].set(top_value)


def block_scale(stream_key, dims, shards, low, top_value):
    level = 1.0
    for axis_at, blocks in shards:
        draws = jax.random.uniform(jax.random.fold_in(jax.random.fold_in(stream_key, 6), axis_at), (blocks,), jnp.float32, low / len(shards), top_value / len(shards))
        level = level * jnp.repeat(jnp.exp(draws), dims[axis_at] // blocks).reshape((-1,) + (1,) * (len(dims) - 1 - axis_at))
    return level


def centred(stream_key, dims, scale, most, shards=(), kind=jnp.bfloat16):
    loudness = block_scale(stream_key, dims, shards, -0.22, 0.18) if shards else 1.0
    array = jax.random.normal(stream_key, dims, jnp.float32) * scale * loudness
    return jnp.minimum(jnp.maximum(array, -most), most).astype(kind)


def setup_inputs(seed: int = 0) -> dict:
    seeds = jax.random.split(jax.random.key(seed), 7)
    initial_field = centred(seeds[0], (NZ, NX, NY), 6.0, 36.0, ((0, 2), (1, 2), (2, 32)), jnp.float32)
    plane_coupling = jnp.clip(jnp.exp(math.log(0.24) - 1.3862944 * jax.random.uniform(seeds[1], (NZ, NX, NY), jnp.float32) ** block_scale(seeds[1], (NZ, NX, NY), ((0, 2), (1, 2), (2, 32)), -0.2, 0.2)), 0.06, 0.24)
    line_coupling = jnp.clip(jnp.exp(math.log(8000.0) - 2.0794415 * jax.random.uniform(seeds[2], (NZ, NX, NY), jnp.float32) ** block_scale(seeds[2], (NZ, NX, NY), ((0, 2), (1, 2), (2, 32)), -0.2, 0.2)), 1000.0, 8000.0)
    source = draw_source(jax.random.fold_in(seeds[6], 71), 0)
    shift_table = jnp.clip(jax.random.uniform(seeds[4], (SHIFTS,), jnp.float32, 0.5, 1.0), 0.5, 1.0)
    shift_index = place_ends(jax.random.randint(seeds[5], (HALF,), 0, SHIFTS), jax.random.fold_in(seeds[5], 1), 0, SHIFTS - 1).astype(jnp.int32)
    return {"initial_field": initial_field, "plane_coupling": plane_coupling, "line_coupling": line_coupling, "source": source, "shift_table": shift_table, "shift_index": shift_index}


def lookup(shift_table, table_row):
    table_slots = jnp.arange(shift_table.shape[0], dtype=jnp.int32)
    return jnp.sum(jnp.where(table_slots == table_row, shift_table, jnp.zeros_like(shift_table)))


def plane_apply(current, coupling):
    padded = jnp.pad(current, ((0, 0), (1, 1), (1, 1)))
    beside_all = padded[:, 2:, 1:-1] + padded[:, :-2, 1:-1] + padded[:, 1:-1, 2:] + padded[:, 1:-1, :-2]
    return coupling * (beside_all - 4.0 * current)


def line_solve(explicit, line_coupling, shift_value):
    scaled = shift_value * line_coupling
    center = 1.0 + 2.0 * scaled

    def forward(previous, inputs):
        before_c, before_d = previous
        coupling, middle, right_side = inputs
        pivot_value = middle + coupling * before_c
        next_c = -coupling / pivot_value
        next_d = (right_side + coupling * before_d) / pivot_value
        return (next_c, next_d), (next_c, next_d)

    zero_plane = jnp.zeros_like(explicit[0])
    final_state, factors = lax.scan(forward, (zero_plane, zero_plane), (scaled, center, explicit))

    def backward(later_value, inputs):
        ratio, offset = inputs
        own_value = offset - ratio * later_value
        return own_value, own_value

    final_value, solved = lax.scan(backward, zero_plane, factors, reverse=True)
    return solved


def reference(initial_field, plane_coupling, line_coupling, source, shift_table, shift_index):
    current = initial_field
    for half_step in range(HALF):
        shift_value = lookup(shift_table, shift_index[half_step])
        explicit = current + shift_value * (plane_apply(current, plane_coupling) + source)
        current = line_solve(explicit, line_coupling, shift_value)
    return current
```

```python
import functools

import jax
import jax.numpy as jnp
from jax import lax
from jax.experimental import pallas as pl
from jax.experimental.pallas import tpu as pltpu
from jax.sharding import PartitionSpec as P


CORE = 1
EDGE_AT = 2
EXPLICIT = 16
BEHIND = 32
FACTOR = 8
SLOTS = 16
WIDTH = 8


def loop(count, body, init, unroll, reverse=False):
    while count % unroll:
        unroll -= 1

    def block(i, carry):
        for j in range(unroll):
            k = i * unroll + j
            carry = body(count - 1 - k if reverse else k, carry)
        return carry

    return lax.fori_loop(0, count // unroll, block, init)


def tree(items, slot):
    bit = 0
    while len(items) > 1:
        odd = (slot >> bit) & 1 == 1
        items = [jnp.where(odd, b, a) for a, b in zip(items[::2], items[1::2])]
        bit += 1
    return items[0]


def kernel(
    ny_parts, half,
    u_in, pc_in, lc_in, src_in, table, index,
    out,
    u_x, pc_x, lc_x, src_x, rl_s, p_s, b_s, f_s, t_s,
    un_s, tr_s, pr_s, un_r, tr_r, pr_r, beta_s, beta_r, iq_s, iq_r, face_s, face_r,
    pk, yk, eo, en, eu, epc, elc, esrc, erl, ep, eb, ef, ret_s, ret_r,
    in_sem, un_sem, tr_ss, tr_rs, pr_ss, pr_rs, be_ss, be_rs, iq_ss, iq_rs, fa_ss, fa_rs,
    y_ss, y_rs, e_ss, e_rs, ret_ss, ret_rs,
):
    n, rows, lanes = u_in.shape
    last = half - 1
    groups = n // SLOTS
    gz, gx, gy = lax.axis_index("gz"), lax.axis_index("gx"), lax.axis_index("gy")
    has_left, has_right = gy > 0, gy < ny_parts - 1
    owner = gx == CORE
    lefts_there = (gy + ny_parts - 1) // ny_parts
    rights_there = (2 * ny_parts - 2 - gy) // ny_parts
    there = (lefts_there, rights_there)
    sides = (lax.rem(gy + ny_parts - 1, ny_parts), lax.rem(gy + 1, ny_parts))
    at_z, at_x = (1 - gz, gz), (1 - gx, gx)
    has_side = at_z[0] * lefts_there + at_z[1] * rights_there == 1
    me = 2 * gz + gx
    full = (rows, lanes)

    loads = [
        pltpu.make_async_copy(i, x, in_sem.at[a])
        for a, (i, x) in enumerate(((u_in, u_x), (pc_in, pc_x), (lc_in, lc_x), (src_in, src_x)))
    ]
    for a in (2, 0, 1, 3):
        loads[a].start()

    barrier = pltpu.get_barrier_semaphore()

    def greet(device):
        pl.semaphore_signal(
            barrier, inc=1, device_id=device, device_id_type=pl.DeviceIdType.MESH
        )

    def when_side(act):
        for s in range(2):

            @pl.when(at_x[CORE] * at_z[s] * there[s] == 1)
            def _(s=s):
                act(sides[s])

    def greet_side(side):
        for q in range(4):
            greet((q // 2, q % 2, side))

    when_side(greet_side)

    z_peer, x_peer, d_peer = (1 - gz, gx, gy), (gz, 1 - gx, gy), (1 - gz, 1 - gx, gy)
    peers = (z_peer, x_peer, d_peer)
    for peer in peers:
        greet(peer)

    def remote(src, dst, send, recv, device):
        return pltpu.make_async_remote_copy(
            src_ref=src, dst_ref=dst, send_sem=send, recv_sem=recv,
            device_id=device, device_id_type=pl.DeviceIdType.MESH,
        )

    def layer(k):
        return k + gz * (n - 1 - 2 * k)

    def shift(h):
        return table[index[h]]

    def inverse(h):
        return 1.0 / jnp.full(full, shift(h), jnp.float32)

    lane = lax.broadcasted_iota(jnp.int32, full, 1)
    row = lax.broadcasted_iota(jnp.int32, full, 0)

    is_low = gx == 0

    def edge(x):
        return jnp.where(is_low, x[rows - 1:rows], x[0:1])

    def factor(coupling, p_ref, b_ref, rl_ref, hs, make, row_ref=None):
        inv = [inverse(h) for h in hs]
        one = jnp.ones(full, jnp.float32)

        def body(k, carry):
            if make:
                rl = 1.0 / coupling(k)
                rl_ref[k] = rl
            else:
                rl = rl_ref[k]
            done = []
            for (p, d), h, i in zip(carry, hs, inv):
                d = d + (rl * i) * p
                q = p + d
                p_ref[h, k] = p
                if row_ref is not None and h < last:
                    row_ref[h, k] = edge(p)
                b_ref[h, k] = 1.0 / (p * q)
                done.append((q, d))
            return tuple(done)

        final = loop(n, body, tuple((one, one) for _ in hs), FACTOR)
        ends = []
        for q, d in final:
            iq = 1.0 / q
            ends.append((iq, d * iq))
        return ends

    def meet(face, beta, iq, face_n, beta_n):
        gain = iq / (beta + beta_n - beta * beta_n)
        return (face_n + (1.0 - beta_n) * face) * gain

    loads[2].wait()
    ends = factor(lambda k: lc_x[layer(k)], p_s, b_s, rl_s, [0], True, pr_s)
    iqs = [e[0] for e in ends]
    iq_s[0] = ends[0][0]
    beta_s[0] = ends[0][1]

    for a in (0, 1, 3):
        loads[a].wait()

    base = 64 * gz + 16 * gx
    low = lane % WIDTH < WIDTH // 2
    fields = (u_x, pc_x, lc_x, src_x)

    def pack(pair, carry):
        for a, e in enumerate(fields):
            packed = []
            for s in range(2):
                g = 2 * pair + s
                moved = []
                for j in range(SLOTS):
                    x = e[layer(g * SLOTS + j)]
                    if a == 0:
                        un_s[g * SLOTS + j] = edge(x)
                    moved.append(pltpu.roll(x, (4 + 8 * j + 4 * s) % lanes, 1))
                at_left = ((lane - 4 - 4 * s) & (lanes - 1)) // WIDTH
                at_right = ((lane + 4 - 4 * s) & (lanes - 1)) // WIDTH
                l = pltpu.roll(tree(moved, at_left), base, 1)
                r = pltpu.roll(tree(moved, at_right), base, 1)
                pk[0, a * groups + g] = l
                pk[1, a * groups + g] = r
                packed.append((l, r))
            (l0, r0), (l1, r1) = packed
            yk[0, a * (groups // 2) + pair] = jnp.where(low, l1, l0)
            yk[1, a * (groups // 2) + pair] = jnp.where(low, r0, r1)
        return carry

    lax.fori_loop(0, groups // 2, pack, 0)

    pl.semaphore_wait(barrier, 3 + lefts_there + rights_there)

    def to_left(q):
        return remote(yk.at[0], en.at[q], y_ss.at[0], y_rs.at[q], (1, CORE, sides[0]))

    def to_right(q):
        return remote(yk.at[1], en.at[q], y_ss.at[1], y_rs.at[q], (0, CORE, sides[1]))

    for q in range(4):

        here = at_z[q // 2] * at_x[q % 2]

        @pl.when(here * lefts_there == 1)
        def _(q=q):
            to_left(q).start()

        @pl.when(here * rights_there == 1)
        def _(q=q):
            to_right(q).start()

    un = remote(un_s, un_r, un_sem.at[0], un_sem.at[1], x_peer)
    un.start()

    def send_betas(h):
        for s, peer in enumerate(peers):
            if s == 0 or h < last:
                c = remote(beta_s.at[h], beta_r.at[h, s], be_ss.at[3 * h + s], be_rs.at[3 * h + s], peer)
                c.start()
                betas[h].append(c)
        if h < last:
            c = remote(iq_s.at[h], iq_r.at[h], iq_ss.at[h], iq_rs.at[h], x_peer)
            c.start()
            betas[h].append(c)
            c = remote(pr_s.at[h], pr_r.at[h], pr_ss.at[h], pr_rs.at[h], x_peer)
            c.start()
            betas[h].append(c)

    betas = [[] for _ in range(half)]
    send_betas(0)

    def to_owner(s, q):
        return remote(pk.at[s], eo.at[q], e_ss.at[s], e_rs.at[q], (s, CORE, gy))

    for q in range(4):
        for s in range(2):
            if q != 2 * s + CORE:

                @pl.when(me == q)
                def _(s=s, q=q):
                    to_owner(s, q).start()

    top_in, bottom_in = gx == 1, gx == 0

    def beside_own(u, other):
        up = jnp.where(row == 0, jnp.where(top_in, other, 0.0), pltpu.roll(u, 1, 0))
        down = jnp.where(
            row == rows - 1, jnp.where(bottom_in, other, 0.0), pltpu.roll(u, rows - 1, 0)
        )
        return (up + down) + (pltpu.roll(u, 1, 1) + pltpu.roll(u, lanes - 1, 1))

    def spread(r):
        return jnp.broadcast_to(r, full)

    def explicit_own(h, v, vn):
        inv = inverse(h)

        def body(k, total):
            z = layer(k)
            if h == 0:
                u, other = u_x[z], spread(un_r[k])
            else:
                u = p_s[h - 1, k] * (v + t_s[k])
                other = spread(pr_r[h - 1, k]) * (vn + spread(tr_r[h - 1, k]))
            e = inv * u + pc_x[z] * (beside_own(u, other) - 4.0 * u) + src_x[z]
            total = total + (p_s[h, k] * rl_s[k]) * e
            f_s[k] = total * b_s[h, k]
            return total

        return loop(n, body, jnp.zeros(full, jnp.float32), EXPLICIT)

    def behind_own(send):
        def body(k, total):
            total = total + f_s[k]
            t_s[k] = total
            if send:
                tr_s[k] = edge(total)
            return total

        loop(n, body, jnp.zeros(full, jnp.float32), BEHIND, reverse=True)

    shifted = lane + 4 * gz

    def edge_wait():
        def waiting(slot, ref, sems):
            remote(ref.at[slot], ref.at[slot], e_ss.at[0], sems.at[slot], x_peer).wait_recv()

        def wait_side(side):
            for slot in range(4):
                waiting(slot, en, y_rs)

        for s in range(2):

            @pl.when(at_x[CORE] * at_z[s] == 1)
            def _(s=s):
                for i in range(4 * groups):
                    eo[2 * s + CORE, i] = pk[s, i]
                for slot in range(4):
                    if slot != 2 * s + CORE:
                        waiting(slot, eo, e_rs)

        when_side(wait_side)

    def edge_unpack():

        filler = lc_x[0]
        zero = jnp.zeros(full, jnp.float32)
        targets = (eu, epc, elc, esrc)

        def unpack(pair, carry):
            for a, e in enumerate(targets):
                rest = filler if a == 2 else zero
                near = [
                    jnp.where(has_side, en[q, a * (groups // 2) + pair], rest) for q in range(4)
                ]
                for s in range(2):
                    g = 2 * pair + s
                    mine = [eo[q, a * groups + g] for q in range(4)]
                    both = {}
                    for m in range(4):
                        x = (shifted - 8 * m - 4 * s) & (lanes - 1)
                        rg = (x // 16) & 1 == 1
                        rel = x & 15
                        from_near = jnp.where(
                            gz == 0, (rel < 4).astype(jnp.int32),
                            ((rel >= 8) & (rel < 12)).astype(jnp.int32),
                        ) == 1
                        for zh in range(2):
                            o = jnp.where(rg, mine[2 * zh + 1], mine[2 * zh])
                            w = jnp.where(rg, near[2 * zh + 1], near[2 * zh])
                            both[m, zh] = jnp.where(from_near, w, o)
                    for j in range(SLOTS):
                        x = (shifted - 8 * j - 4 * s) & (lanes - 1)
                        v = jnp.where(x >= 64, both[j % 4, 1], both[j % 4, 0])
                        e[g * SLOTS + j] = pltpu.roll(v, (lanes - 8 * j - 4 * s) % lanes, 1)
            return carry

        lax.fori_loop(0, groups // 2, unpack, 0)

    def edges():
        edge_unpack()
        ends = factor(lambda k: elc[k], ep, eb, erl, list(range(half)), True)
        in_second = (shifted // 16) & 1 == 1
        top, bottom = row == 0, row == rows - 1
        for h in range(half):
            inv = inverse(h)

            def explicit(k, total, h=h, inv=inv):
                u = eu[k]
                up, down = pltpu.roll(u, 1, 0), pltpu.roll(u, rows - 1, 0)
                up = jnp.where(
                    top, jnp.where(in_second, pltpu.roll(up, 16, 1), 0.0), up
                )
                down = jnp.where(
                    bottom, jnp.where(in_second, 0.0, pltpu.roll(down, lanes - 16, 1)), down
                )
                beside = (up + down) + (pltpu.roll(u, 1, 1) + pltpu.roll(u, lanes - 1, 1))
                e = inv * u + epc[k] * (beside - 4.0 * u) + esrc[k]
                total = total + (ep[h, k] * erl[k]) * e
                ef[k] = total * eb[h, k]
                return total

            total = loop(n, explicit, jnp.zeros(full, jnp.float32), EXPLICIT)
            iq, beta = ends[h]
            face = total * iq
            v = meet(face, beta, iq, pltpu.roll(face, 64, 1), pltpu.roll(beta, 64, 1))

            def behind(k, total, h=h):
                total = total + ef[k]
                eu[k] = ep[h, k] * total
                return total

            loop(n, behind, v, BEHIND, reverse=True)

        def give(g, carry):
            moved = [pltpu.roll(eu[g * SLOTS + j], 8 * j, 1) for j in range(SLOTS)]
            for q in range(4):
                at = (lane // WIDTH - 8 * (q // 2) - 2 * (q % 2)) & (SLOTS - 1)
                b = 64 * (q // 2) + 16 * (q % 2)
                ret_s[q, g] = pltpu.roll(tree(moved, at), (lanes - b) % lanes, 1)
            return carry

        lax.fori_loop(0, groups, give, 0)
        for s in range(2):

            @pl.when(gz == s)
            def _(s=s):
                for q in range(4):
                    if q != 2 * s + CORE:
                        remote(
                            ret_s.at[q], ret_r.at[s], ret_ss.at[q], ret_rs.at[s],
                            (q // 2, q % 2, gy),
                        ).start()
                for g in range(groups):
                    ret_r[s, g] = ret_s[2 * s + CORE, g]

    un.wait()
    v = vn = None
    faces = []
    tails = []
    for h in range(half):
        total = explicit_own(h, v, vn)
        face = total * iq_s[h]
        face_s[h] = face
        sends = []
        for s, peer in enumerate(peers):
            if s == 0 or h < last:
                c = remote(face_s.at[h], face_r.at[h, s], fa_ss.at[3 * h + s], fa_rs.at[3 * h + s], peer)
                c.start()
                sends.append(c)
        faces.append(sends)
        if h == 0:
            hs = list(range(1, half))
            for i, (iq, beta) in zip(hs, factor(None, p_s, b_s, rl_s, hs, False, pr_s)):
                iq_s[i] = iq
                beta_s[i] = beta
        behind_own(h < last)
        if h < last:
            c = remote(tr_s, tr_r.at[h], tr_ss.at[h], tr_rs.at[h], x_peer)
            c.start()
            tails.append(c)
        if h == 0:
            for i in hs:
                send_betas(i)
        if h == EDGE_AT:

            edge_wait()

            @pl.when(owner)
            def _():
                edges()

        for c in betas[h]:
            c.wait()
        if h < last:
            tails[h].wait()
        for c in sends:
            c.wait()
        iq, beta = iq_s[h], beta_s[h]
        v = meet(face_s[h], beta, iq, face_r[h, 0], beta_r[h, 0])
        if h < last:
            w = meet(face_r[h, 1], beta_r[h, 1], iq_r[h], face_r[h, 2], beta_r[h, 2])
            vn = jnp.where(is_low, spread(w[0:1]), spread(w[rows - 1:rows]))

    for s in range(2):

        @pl.when(me != 2 * s + CORE)
        def _(s=s):
            remote(
                ret_s.at[0], ret_r.at[s], ret_ss.at[0], ret_rs.at[s], x_peer
            ).wait_recv()

    outer = (lane < 4) | (lane >= lanes - 4)

    def write(g, carry):
        both = jnp.where(low, ret_r[1, g], ret_r[0, g])
        for j in range(SLOTS):
            k = g * SLOTS + j
            u = p_s[last, k] * (v + t_s[k])
            out[layer(k)] = jnp.where(outer, pltpu.roll(both, (lanes - 4 - 8 * j) % lanes, 1), u)
        return carry

    lax.fori_loop(0, groups, write, 0)

    @pl.when(has_left)
    def _():
        to_left(0).wait_send()

    @pl.when(has_right)
    def _():
        to_right(0).wait_send()

    for s in range(2):

        @pl.when(me != 2 * s + CORE)
        def _(s=s):
            to_owner(s, 0).wait_send()

    @pl.when(owner)
    def _():
        for q in range(4):

            @pl.when(me != q)
            def _(q=q):
                remote(
                    ret_s.at[q], ret_r.at[0], ret_ss.at[q], ret_rs.at[0], x_peer
                ).wait_send()


def solution(mesh):
    ny_parts = mesh.shape["gy"]
    assert mesh.shape["gz"] == 2 and mesh.shape["gx"] == 2

    def on_device(u, pc, lc, src, table, index):
        half = index.shape[0]
        n, rows, lanes = u.shape
        groups = n // SLOTS
        assert (rows, lanes, half) == (8, 128, 4) and n % (2 * SLOTS) == 0

        def vmem(*dims):
            return pltpu.VMEM(dims, jnp.float32)

        def tiles(*dims):
            return vmem(*dims, rows, lanes)

        dma = pltpu.SemaphoreType.DMA
        scratch = [tiles(n)] * 5 + [tiles(half, n)] * 2 + [tiles(n)] * 2
        scratch += [vmem(n, 1, lanes), vmem(n, 1, lanes), vmem(half - 1, n, 1, lanes)]
        scratch += [vmem(n, 1, lanes), vmem(half - 1, n, 1, lanes), vmem(half - 1, n, 1, lanes)]
        scratch += [tiles(half), tiles(half, 3), tiles(half), tiles(half - 1)]
        scratch += [tiles(half), tiles(half, 3)]
        scratch += [tiles(2, 4 * groups), tiles(2, 2 * groups), tiles(4, 4 * groups), tiles(4, 2 * groups)]
        scratch += [tiles(n)] * 5 + [tiles(half, n)] * 2 + [tiles(n)]
        scratch += [tiles(4, groups), tiles(2, groups)]
        scratch += [dma((4,)), dma((2,))]
        scratch += [dma((half - 1,))] * 4
        scratch += [dma((3 * half,))] * 2
        scratch += [dma((half - 1,))] * 2
        scratch += [dma((3 * half,))] * 2
        scratch += [dma((2,)), dma((4,)), dma((2,)), dma((4,)), dma((4,)), dma((2,))]
        return pl.pallas_call(
            functools.partial(kernel, ny_parts, half),
            out_shape=pltpu.VMEM(u.shape, jnp.float32),
            in_specs=[pl.BlockSpec(memory_space=pl.ANY)] * 4
            + [pl.BlockSpec(memory_space=pltpu.SMEM)] * 2,
            out_specs=pl.BlockSpec(memory_space=pltpu.VMEM),
            scratch_shapes=scratch,
            compiler_params=pltpu.CompilerParams(collective_id=0, has_side_effects=True),
        )(u, pc, lc, src, table, index)

    spec = P("gz", "gx", "gy")
    return jax.shard_map(
        on_device, mesh=mesh, in_specs=(spec,) * 4 + (P(), P()), out_specs=spec, check_vma=False
    )
```

```python
import functools

import jax
import jax.numpy as jnp
from jax import lax
from jax.experimental import pallas as pl
from jax.experimental.pallas import tpu as pltpu
from jax.sharding import PartitionSpec as P


CORE = 1
EDGE_AT = 2
EXPLICIT = 16
BEHIND = 32
FACTOR = 8
SLOTS = 16
WIDTH = 8


def loop(count, body, init, unroll, reverse=False):
    while count % unroll:
        unroll -= 1

    def block(i, carry):
        for j in range(unroll):
            k = i * unroll + j
            carry = body(count - 1 - k if reverse else k, carry)
        return carry

    return lax.fori_loop(0, count // unroll, block, init)


def tree(items, slot):
    bit = 0
    while len(items) > 1:
        odd = (slot >> bit) & 1 == 1
        items = [jnp.where(odd, b, a) for a, b in zip(items[::2], items[1::2])]
        bit += 1
    return items[0]


def kernel(
    ny_parts, half,
    u_in, pc_in, lc_in, src_in, table, index,
    out,
    u_x, pc_x, lc_x, src_x, rl_s, p_s, b_s, f_s, t_s,
    un_s, tr_s, pr_s, un_r, tr_r, pr_r, beta_s, beta_r, iq_s, iq_r, face_s, face_r,
    pk, yk, eo, en, eu, epc, elc, esrc, erl, ep, eb, ef, ret_s, ret_r,
    in_sem, un_sem, tr_ss, tr_rs, pr_ss, pr_rs, be_ss, be_rs, iq_ss, iq_rs, fa_ss, fa_rs,
    group_sem, far_sem, y_ss, y_rs, e_ss, e_rs, ret_ss, ret_rs,
):
    n, rows, lanes = u_in.shape
    last = half - 1
    groups = n // SLOTS
    gz, gx, gy = lax.axis_index("gz"), lax.axis_index("gx"), lax.axis_index("gy")
    has_left, has_right = gy > 0, gy < ny_parts - 1
    owner = gx == CORE
    lefts_there = (gy + ny_parts - 1) // ny_parts
    rights_there = (2 * ny_parts - 2 - gy) // ny_parts
    there = (lefts_there, rights_there)
    sides = (lax.rem(gy + ny_parts - 1, ny_parts), lax.rem(gy + 1, ny_parts))
    at_z, at_x = (1 - gz, gz), (1 - gx, gx)
    has_side = at_z[0] * lefts_there + at_z[1] * rights_there == 1
    me = 2 * gz + gx
    full = (rows, lanes)

    loads = [
        pltpu.make_async_copy(i, x, in_sem.at[a])
        for a, (i, x) in enumerate(((u_in, u_x), (pc_in, pc_x), (lc_in, lc_x), (src_in, src_x)))
    ]
    for a in (2, 0, 1, 3):
        loads[a].start()

    barrier = pltpu.get_barrier_semaphore()

    def greet(device):
        pl.semaphore_signal(
            barrier, inc=1, device_id=device, device_id_type=pl.DeviceIdType.MESH
        )

    z_peer, x_peer, d_peer = (1 - gz, gx, gy), (gz, 1 - gx, gy), (1 - gz, 1 - gx, gy)
    peers = (z_peer, x_peer, d_peer)
    for peer in peers:
        greet(peer)

    def when_side(act):
        for s in range(2):

            @pl.when(at_x[CORE] * at_z[s] * there[s] == 1)
            def _(s=s):
                act(s)

    when_side(lambda s: greet((1 - s, CORE, sides[s])))

    def remote(src, dst, send, recv, device):
        return pltpu.make_async_remote_copy(
            src_ref=src, dst_ref=dst, send_sem=send, recv_sem=recv,
            device_id=device, device_id_type=pl.DeviceIdType.MESH,
        )

    def layer(k):
        return k + gz * (n - 1 - 2 * k)

    def shift(h):
        return table[index[h]]

    def inverse(h):
        return 1.0 / jnp.full(full, shift(h), jnp.float32)

    lane = lax.broadcasted_iota(jnp.int32, full, 1)
    row = lax.broadcasted_iota(jnp.int32, full, 0)

    is_low = gx == 0

    def edge(x):
        return jnp.where(is_low, x[rows - 1:rows], x[0:1])

    def factor(coupling, p_ref, b_ref, rl_ref, hs, make, row_ref=None):
        inv = [inverse(h) for h in hs]
        one = jnp.ones(full, jnp.float32)

        def body(k, carry):
            if make:
                rl = 1.0 / coupling(k)
                rl_ref[k] = rl
            else:
                rl = rl_ref[k]
            done = []
            for (p, d), h, i in zip(carry, hs, inv):
                d = d + (rl * i) * p
                q = p + d
                p_ref[h, k] = p
                if row_ref is not None and h < last:
                    row_ref[h, k] = edge(p)
                b_ref[h, k] = 1.0 / (p * q)
                done.append((q, d))
            return tuple(done)

        final = loop(n, body, tuple((one, one) for _ in hs), FACTOR)
        ends = []
        for q, d in final:
            iq = 1.0 / q
            ends.append((iq, d * iq))
        return ends

    def meet(face, beta, iq, face_n, beta_n):
        gain = iq / (beta + beta_n - beta * beta_n)
        return (face_n + (1.0 - beta_n) * face) * gain

    loads[2].wait()
    ends = factor(lambda k: lc_x[layer(k)], p_s, b_s, rl_s, [0], True, pr_s)
    iqs = [e[0] for e in ends]
    iq_s[0] = ends[0][0]
    beta_s[0] = ends[0][1]

    for a in (0, 1, 3):
        loads[a].wait()

    base = 64 * gz + 16 * gx
    low = lane % WIDTH < WIDTH // 2
    fields = (u_x, pc_x, lc_x, src_x)

    def pack(pair, carry):
        for a, e in enumerate(fields):
            packed = []
            for s in range(2):
                g = 2 * pair + s
                moved = []
                for j in range(SLOTS):
                    x = e[layer(g * SLOTS + j)]
                    if a == 0:
                        un_s[g * SLOTS + j] = edge(x)
                    moved.append(pltpu.roll(x, (4 + 8 * j + 4 * s) % lanes, 1))
                at_left = ((lane - 4 - 4 * s) & (lanes - 1)) // WIDTH
                at_right = ((lane + 4 - 4 * s) & (lanes - 1)) // WIDTH
                l = pltpu.roll(tree(moved, at_left), base, 1)
                r = pltpu.roll(tree(moved, at_right), base, 1)
                pk[0, a * groups + g] = l
                pk[1, a * groups + g] = r
                packed.append((l, r))
            (l0, r0), (l1, r1) = packed
            yk[0, a * (groups // 2) + pair] = jnp.where(low, l1, l0)
            yk[1, a * (groups // 2) + pair] = jnp.where(low, r0, r1)
        return carry

    lax.fori_loop(0, groups // 2, pack, 0)

    def tell(sem, device):
        pl.semaphore_signal(sem, inc=1, device_id=device, device_id_type=pl.DeviceIdType.MESH)

    @pl.when(gx != CORE)
    def _():
        pl.semaphore_wait(barrier, 3)
        tell(group_sem, x_peer)

    @pl.when(gx == CORE)
    def _():
        pl.semaphore_wait(group_sem, 1)

    def to_side(s, q):
        return remote(yk.at[s], en.at[q], y_ss.at[s], y_rs.at[q], (1 - s, CORE, sides[s]))

    un = remote(un_s, un_r, un_sem.at[0], un_sem.at[1], x_peer)
    un.start()

    def send_betas(h):
        for s, peer in enumerate(peers):
            if s == 0 or h < last:
                c = remote(beta_s.at[h], beta_r.at[h, s], be_ss.at[3 * h + s], be_rs.at[3 * h + s], peer)
                c.start()
                betas[h].append(c)
        if h < last:
            c = remote(iq_s.at[h], iq_r.at[h], iq_ss.at[h], iq_rs.at[h], x_peer)
            c.start()
            betas[h].append(c)
            c = remote(pr_s.at[h], pr_r.at[h], pr_ss.at[h], pr_rs.at[h], x_peer)
            c.start()
            betas[h].append(c)

    betas = [[] for _ in range(half)]
    send_betas(0)

    def to_owner(s, q):
        return remote(pk.at[s], eo.at[q], e_ss.at[s], e_rs.at[q], (s, CORE, gy))

    for q in range(4):
        for s in range(2):
            if q != 2 * s + CORE:

                @pl.when(me == q)
                def _(s=s, q=q):
                    to_owner(s, q).start()

    top_in, bottom_in = gx == 1, gx == 0

    def beside_own(u, other):
        up = jnp.where(row == 0, jnp.where(top_in, other, 0.0), pltpu.roll(u, 1, 0))
        down = jnp.where(
            row == rows - 1, jnp.where(bottom_in, other, 0.0), pltpu.roll(u, rows - 1, 0)
        )
        return (up + down) + (pltpu.roll(u, 1, 1) + pltpu.roll(u, lanes - 1, 1))

    def spread(r):
        return jnp.broadcast_to(r, full)

    def explicit_own(h, v, vn):
        inv = inverse(h)

        def body(k, total):
            z = layer(k)
            if h == 0:
                u, other = u_x[z], spread(un_r[k])
            else:
                u = p_s[h - 1, k] * (v + t_s[k])
                other = spread(pr_r[h - 1, k]) * (vn + spread(tr_r[h - 1, k]))
            e = inv * u + pc_x[z] * (beside_own(u, other) - 4.0 * u) + src_x[z]
            total = total + (p_s[h, k] * rl_s[k]) * e
            f_s[k] = total * b_s[h, k]
            return total

        return loop(n, body, jnp.zeros(full, jnp.float32), EXPLICIT)

    def behind_own(send):
        def body(k, total):
            total = total + f_s[k]
            t_s[k] = total
            if send:
                tr_s[k] = edge(total)
            return total

        loop(n, body, jnp.zeros(full, jnp.float32), BEHIND, reverse=True)

    shifted = lane + 4 * gz

    def edge_wait():
        def waiting(slot, ref, sems):
            remote(ref.at[slot], ref.at[slot], e_ss.at[0], sems.at[slot], x_peer).wait_recv()

        def wait_side(s):
            for slot in range(4):
                waiting(slot, en, y_rs)

        for s in range(2):

            @pl.when(at_x[CORE] * at_z[s] == 1)
            def _(s=s):
                for i in range(4 * groups):
                    eo[2 * s + CORE, i] = pk[s, i]
                for slot in range(4):
                    if slot != 2 * s + CORE:
                        waiting(slot, eo, e_rs)

        when_side(wait_side)

    def far_sends():
        @pl.when(gx == CORE)
        def _():
            pl.semaphore_wait(barrier, 3 + at_z[0] * lefts_there + at_z[1] * rights_there)

        def relay(s):
            for peer in peers:
                tell(far_sem.at[s], peer)

        when_side(relay)
        for q in range(4):
            for s in range(2):
                here = at_z[q // 2] * at_x[q % 2] * there[s]

                @pl.when(here == 1)
                def _(q=q, s=s):
                    if q != 2 * s + CORE:
                        pl.semaphore_wait(far_sem.at[s], 1)
                    to_side(s, q).start()

    def edge_unpack():

        filler = lc_x[0]
        zero = jnp.zeros(full, jnp.float32)
        targets = (eu, epc, elc, esrc)

        def unpack(pair, carry):
            for a, e in enumerate(targets):
                rest = filler if a == 2 else zero
                near = [
                    jnp.where(has_side, en[q, a * (groups // 2) + pair], rest) for q in range(4)
                ]
                for s in range(2):
                    g = 2 * pair + s
                    mine = [eo[q, a * groups + g] for q in range(4)]
                    both = {}
                    for m in range(4):
                        x = (shifted - 8 * m - 4 * s) & (lanes - 1)
                        rg = (x // 16) & 1 == 1
                        rel = x & 15
                        from_near = jnp.where(
                            gz == 0, (rel < 4).astype(jnp.int32),
                            ((rel >= 8) & (rel < 12)).astype(jnp.int32),
                        ) == 1
                        for zh in range(2):
                            o = jnp.where(rg, mine[2 * zh + 1], mine[2 * zh])
                            w = jnp.where(rg, near[2 * zh + 1], near[2 * zh])
                            both[m, zh] = jnp.where(from_near, w, o)
                    for j in range(SLOTS):
                        x = (shifted - 8 * j - 4 * s) & (lanes - 1)
                        v = jnp.where(x >= 64, both[j % 4, 1], both[j % 4, 0])
                        e[g * SLOTS + j] = pltpu.roll(v, (lanes - 8 * j - 4 * s) % lanes, 1)
            return carry

        lax.fori_loop(0, groups // 2, unpack, 0)

    def edges():
        edge_unpack()
        ends = factor(lambda k: elc[k], ep, eb, erl, list(range(half)), True)
        in_second = (shifted // 16) & 1 == 1
        top, bottom = row == 0, row == rows - 1
        for h in range(half):
            inv = inverse(h)

            def explicit(k, total, h=h, inv=inv):
                u = eu[k]
                up, down = pltpu.roll(u, 1, 0), pltpu.roll(u, rows - 1, 0)
                up = jnp.where(
                    top, jnp.where(in_second, pltpu.roll(up, 16, 1), 0.0), up
                )
                down = jnp.where(
                    bottom, jnp.where(in_second, 0.0, pltpu.roll(down, lanes - 16, 1)), down
                )
                beside = (up + down) + (pltpu.roll(u, 1, 1) + pltpu.roll(u, lanes - 1, 1))
                e = inv * u + epc[k] * (beside - 4.0 * u) + esrc[k]
                total = total + (ep[h, k] * erl[k]) * e
                ef[k] = total * eb[h, k]
                return total

            total = loop(n, explicit, jnp.zeros(full, jnp.float32), EXPLICIT)
            iq, beta = ends[h]
            face = total * iq
            v = meet(face, beta, iq, pltpu.roll(face, 64, 1), pltpu.roll(beta, 64, 1))

            def behind(k, total, h=h):
                total = total + ef[k]
                eu[k] = ep[h, k] * total
                return total

            loop(n, behind, v, BEHIND, reverse=True)

        def give(g, carry):
            moved = [pltpu.roll(eu[g * SLOTS + j], 8 * j, 1) for j in range(SLOTS)]
            for q in range(4):
                at = (lane // WIDTH - 8 * (q // 2) - 2 * (q % 2)) & (SLOTS - 1)
                b = 64 * (q // 2) + 16 * (q % 2)
                ret_s[q, g] = pltpu.roll(tree(moved, at), (lanes - b) % lanes, 1)
            return carry

        lax.fori_loop(0, groups, give, 0)
        for s in range(2):

            @pl.when(gz == s)
            def _(s=s):
                for q in range(4):
                    if q != 2 * s + CORE:
                        remote(
                            ret_s.at[q], ret_r.at[s], ret_ss.at[q], ret_rs.at[s],
                            (q // 2, q % 2, gy),
                        ).start()
                for g in range(groups):
                    ret_r[s, g] = ret_s[2 * s + CORE, g]

    un.wait()
    v = vn = None
    faces = []
    tails = []
    for h in range(half):
        total = explicit_own(h, v, vn)
        face = total * iq_s[h]
        face_s[h] = face
        sends = []
        for s, peer in enumerate(peers):
            if s == 0 or h < last:
                c = remote(face_s.at[h], face_r.at[h, s], fa_ss.at[3 * h + s], fa_rs.at[3 * h + s], peer)
                c.start()
                sends.append(c)
        faces.append(sends)
        if h == 0:
            far_sends()
        if h == 0:
            hs = list(range(1, half))
            for i, (iq, beta) in zip(hs, factor(None, p_s, b_s, rl_s, hs, False, pr_s)):
                iq_s[i] = iq
                beta_s[i] = beta
        behind_own(h < last)
        if h < last:
            c = remote(tr_s, tr_r.at[h], tr_ss.at[h], tr_rs.at[h], x_peer)
            c.start()
            tails.append(c)
        if h == 0:
            for i in hs:
                send_betas(i)
        if h == EDGE_AT:

            edge_wait()

            @pl.when(owner)
            def _():
                edges()

        for c in betas[h]:
            c.wait()
        if h < last:
            tails[h].wait()
        for c in sends:
            c.wait()
        iq, beta = iq_s[h], beta_s[h]
        v = meet(face_s[h], beta, iq, face_r[h, 0], beta_r[h, 0])
        if h < last:
            w = meet(face_r[h, 1], beta_r[h, 1], iq_r[h], face_r[h, 2], beta_r[h, 2])
            vn = jnp.where(is_low, spread(w[0:1]), spread(w[rows - 1:rows]))

    for s in range(2):

        @pl.when(me != 2 * s + CORE)
        def _(s=s):
            remote(
                ret_s.at[0], ret_r.at[s], ret_ss.at[0], ret_rs.at[s], x_peer
            ).wait_recv()

    outer = (lane < 4) | (lane >= lanes - 4)

    def write(g, carry):
        both = jnp.where(low, ret_r[1, g], ret_r[0, g])
        for j in range(SLOTS):
            k = g * SLOTS + j
            u = p_s[last, k] * (v + t_s[k])
            out[layer(k)] = jnp.where(outer, pltpu.roll(both, (lanes - 4 - 8 * j) % lanes, 1), u)
        return carry

    lax.fori_loop(0, groups, write, 0)

    @pl.when(has_left)
    def _():
        to_side(0, 0).wait_send()

    @pl.when(has_right)
    def _():
        to_side(1, 0).wait_send()

    for s in range(2):

        @pl.when(me != 2 * s + CORE)
        def _(s=s):
            to_owner(s, 0).wait_send()

    @pl.when(owner)
    def _():
        for q in range(4):

            @pl.when(me != q)
            def _(q=q):
                remote(
                    ret_s.at[q], ret_r.at[0], ret_ss.at[q], ret_rs.at[0], x_peer
                ).wait_send()


def solution(mesh):
    ny_parts = mesh.shape["gy"]
    assert mesh.shape["gz"] == 2 and mesh.shape["gx"] == 2

    def on_device(u, pc, lc, src, table, index):
        half = index.shape[0]
        n, rows, lanes = u.shape
        groups = n // SLOTS
        assert (rows, lanes, half) == (8, 128, 4) and n % (2 * SLOTS) == 0

        def vmem(*dims):
            return pltpu.VMEM(dims, jnp.float32)

        def tiles(*dims):
            return vmem(*dims, rows, lanes)

        dma = pltpu.SemaphoreType.DMA
        scratch = [tiles(n)] * 5 + [tiles(half, n)] * 2 + [tiles(n)] * 2
        scratch += [vmem(n, 1, lanes), vmem(n, 1, lanes), vmem(half - 1, n, 1, lanes)]
        scratch += [vmem(n, 1, lanes), vmem(half - 1, n, 1, lanes), vmem(half - 1, n, 1, lanes)]
        scratch += [tiles(half), tiles(half, 3), tiles(half), tiles(half - 1)]
        scratch += [tiles(half), tiles(half, 3)]
        scratch += [tiles(2, 4 * groups), tiles(2, 2 * groups), tiles(4, 4 * groups), tiles(4, 2 * groups)]
        scratch += [tiles(n)] * 5 + [tiles(half, n)] * 2 + [tiles(n)]
        scratch += [tiles(4, groups), tiles(2, groups)]
        scratch += [dma((4,)), dma((2,))]
        scratch += [dma((half - 1,))] * 4
        scratch += [dma((3 * half,))] * 2
        scratch += [dma((half - 1,))] * 2
        scratch += [dma((3 * half,))] * 2
        scratch += [pltpu.SemaphoreType.REGULAR, pltpu.SemaphoreType.REGULAR((2,))]
        scratch += [dma((2,)), dma((4,)), dma((2,)), dma((4,)), dma((4,)), dma((2,))]
        return pl.pallas_call(
            functools.partial(kernel, ny_parts, half),
            out_shape=pltpu.VMEM(u.shape, jnp.float32),
            in_specs=[pl.BlockSpec(memory_space=pl.ANY)] * 4
            + [pl.BlockSpec(memory_space=pltpu.SMEM)] * 2,
            out_specs=pl.BlockSpec(memory_space=pltpu.VMEM),
            scratch_shapes=scratch,
            compiler_params=pltpu.CompilerParams(collective_id=0, has_side_effects=True),
        )(u, pc, lc, src, table, index)

    spec = P("gz", "gx", "gy")
    return jax.shard_map(
        on_device, mesh=mesh, in_specs=(spec,) * 4 + (P(), P()), out_specs=spec, check_vma=False
    )
```

```python
import functools

import jax
import jax.numpy as jnp
from jax import lax
from jax.experimental import pallas as pl
from jax.experimental.pallas import tpu as pltpu
from jax.sharding import PartitionSpec as P


CORE = 1
EDGE_AT = 2
EDGE_SPLIT = 4
EXPLICIT = 64
BEHIND = 64
CHUNK = 8
FACTOR = 8
SLOTS = 16
WIDTH = 8


def loop(count, body, init, unroll, reverse=False):
    while count % unroll:
        unroll -= 1

    def block(i, carry):
        for j in range(unroll):
            k = i * unroll + j
            carry = body(count - 1 - k if reverse else k, carry)
        return carry

    return lax.fori_loop(0, count // unroll, block, init)


def tree(items, slot):
    bit = 0
    while len(items) > 1:
        odd = (slot >> bit) & 1 == 1
        items = [jnp.where(odd, b, a) for a, b in zip(items[::2], items[1::2])]
        bit += 1
    return items[0]


def kernel(
    ny_parts, half,
    u_in, pc_in, lc_in, src_in, table, index,
    out,
    u_x, pc_x, lc_x, src_x, rl_s, p_s, b_s, f_s, t_s,
    un_s, tr_s, pr_s, un_r, tr_r, pr_r, beta_s, beta_r, iq_s, iq_r, face_s, face_r,
    pk, yk, eo, en, eu, epc, elc, esrc, erl, ep, eb, ef, eiq, ebeta, ret_s, ret_r,
    in_sem, un_sem, tr_ss, tr_rs, pr_ss, pr_rs, be_ss, be_rs, iq_ss, iq_rs, fa_ss, fa_rs,
    group_sem, far_sem, y_ss, y_rs, e_ss, e_rs, ret_ss, ret_rs,
):
    n, rows, lanes = u_in.shape
    last = half - 1
    groups = n // SLOTS
    gz, gx, gy = lax.axis_index("gz"), lax.axis_index("gx"), lax.axis_index("gy")
    has_left, has_right = gy > 0, gy < ny_parts - 1
    owner = gx == CORE
    lefts_there = (gy + ny_parts - 1) // ny_parts
    rights_there = (2 * ny_parts - 2 - gy) // ny_parts
    there = (lefts_there, rights_there)
    sides = (lax.rem(gy + ny_parts - 1, ny_parts), lax.rem(gy + 1, ny_parts))
    at_z, at_x = (1 - gz, gz), (1 - gx, gx)
    side = 1 - gz
    has_side = at_z[1] * lefts_there + at_z[0] * rights_there == 1
    me = 2 * gz + gx
    full = (rows, lanes)

    loads = [
        pltpu.make_async_copy(i, x, in_sem.at[a])
        for a, (i, x) in enumerate(((u_in, u_x), (pc_in, pc_x), (lc_in, lc_x), (src_in, src_x)))
    ]
    for a in (2, 0, 1, 3):
        loads[a].start()

    barrier = pltpu.get_barrier_semaphore()

    def greet(device):
        pl.semaphore_signal(
            barrier, inc=1, device_id=device, device_id_type=pl.DeviceIdType.MESH
        )

    z_peer, x_peer, d_peer = (1 - gz, gx, gy), (gz, 1 - gx, gy), (1 - gz, 1 - gx, gy)
    peers = (z_peer, x_peer, d_peer)
    for peer in peers:
        greet(peer)

    def when_side(act):
        for s in range(2):

            @pl.when(at_x[CORE] * at_z[1 - s] * there[s] == 1)
            def _(s=s):
                act(s)

    when_side(lambda s: greet((s, CORE, sides[s])))

    def remote(src, dst, send, recv, device):
        return pltpu.make_async_remote_copy(
            src_ref=src, dst_ref=dst, send_sem=send, recv_sem=recv,
            device_id=device, device_id_type=pl.DeviceIdType.MESH,
        )

    def layer(k):
        return k + gz * (n - 1 - 2 * k)

    def shift(h):
        return table[index[h]]

    def inverse(h):
        return 1.0 / jnp.full(full, shift(h), jnp.float32)

    lane = lax.broadcasted_iota(jnp.int32, full, 1)
    row = lax.broadcasted_iota(jnp.int32, full, 0)

    is_low = gx == 0

    def edge(x):
        return jnp.where(is_low, x[rows - 1:rows], x[0:1])

    def factor(coupling, p_ref, b_ref, rl_ref, hs, make, row_ref=None):
        inv = [inverse(h) for h in hs]
        one = jnp.ones(full, jnp.float32)

        def body(k, carry):
            if make:
                rl = 1.0 / coupling(k)
                rl_ref[k] = rl
            else:
                rl = rl_ref[k]
            done = []
            for (p, d), h, i in zip(carry, hs, inv):
                add = (rl * i) * p
                q = (p + d) + add
                d = d + add
                p_ref[h, k] = p
                if row_ref is not None and h < last:
                    row_ref[h, k] = edge(p)
                b_ref[h, k] = 1.0 / (p * q)
                done.append((q, d))
            return tuple(done)

        final = loop(n, body, tuple((one, one) for _ in hs), FACTOR)
        ends = []
        for q, d in final:
            iq = 1.0 / q
            ends.append((iq, d * iq))
        return ends

    def meet(face, beta, iq, face_n, beta_n):
        gain = iq / (beta + beta_n - beta * beta_n)
        return (face_n + (1.0 - beta_n) * face) * gain

    loads[2].wait()
    ends = factor(lambda k: lc_x[layer(k)], p_s, b_s, rl_s, [0], True, pr_s)
    iqs = [e[0] for e in ends]
    iq_s[0] = ends[0][0]
    beta_s[0] = ends[0][1]

    for a in (0, 1, 3):
        loads[a].wait()

    base = 16 * gz + 64 * gx
    low = lane % WIDTH < WIDTH // 2
    fields = (u_x, pc_x, lc_x, src_x)

    def pack(pair, carry):
        for a, e in enumerate(fields):
            packed = []
            for s in range(2):
                g = 2 * pair + s
                moved = []
                for j in range(SLOTS):
                    x = e[layer(g * SLOTS + j)]
                    if a == 0:
                        un_s[g * SLOTS + j] = edge(x)
                    moved.append(pltpu.roll(x, (4 + 8 * j + 4 * s) % lanes, 1))
                at_left = ((lane - 4 - 4 * s) & (lanes - 1)) // WIDTH
                at_right = ((lane + 4 - 4 * s) & (lanes - 1)) // WIDTH
                l = pltpu.roll(tree(moved, at_left), base, 1)
                r = pltpu.roll(tree(moved, at_right), base, 1)
                pk[0, a * groups + g] = l
                pk[1, a * groups + g] = r
                packed.append((l, r))
            (l0, r0), (l1, r1) = packed
            yk[0, a * (groups // 2) + pair] = jnp.where(low, l1, l0)
            yk[1, a * (groups // 2) + pair] = jnp.where(low, r0, r1)
        return carry

    lax.fori_loop(0, groups // 2, pack, 0)

    def tell(sem, device):
        pl.semaphore_signal(sem, inc=1, device_id=device, device_id_type=pl.DeviceIdType.MESH)

    @pl.when(gx != CORE)
    def _():
        pl.semaphore_wait(barrier, 3)
        tell(group_sem, x_peer)

    @pl.when(gx == CORE)
    def _():
        pl.semaphore_wait(group_sem, 1)

    def to_side(s, q):
        return remote(yk.at[s], en.at[q], y_ss.at[s], y_rs.at[q], (s, CORE, sides[s]))

    un = remote(un_s, un_r, un_sem.at[0], un_sem.at[1], x_peer)
    un.start()

    def send_betas(h):
        for s, peer in enumerate(peers):
            if s == 0 or h < last:
                c = remote(beta_s.at[h], beta_r.at[h, s], be_ss.at[3 * h + s], be_rs.at[3 * h + s], peer)
                c.start()
                betas[h].append(c)
        if h < last:
            c = remote(iq_s.at[h], iq_r.at[h], iq_ss.at[h], iq_rs.at[h], x_peer)
            c.start()
            betas[h].append(c)
            c = remote(pr_s.at[h], pr_r.at[h], pr_ss.at[h], pr_rs.at[h], x_peer)
            c.start()
            betas[h].append(c)

    betas = [[] for _ in range(half)]
    send_betas(0)

    def to_owner(s, q):
        return remote(pk.at[s], eo.at[q], e_ss.at[s], e_rs.at[q], (1 - s, CORE, gy))

    for q in range(4):
        for s in range(2):
            if q != 2 * (1 - s) + CORE:

                @pl.when(me == q)
                def _(s=s, q=q):
                    to_owner(s, q).start()

    top_in, bottom_in = gx == 1, gx == 0

    def beside_own(u, other):
        up = jnp.where(row == 0, jnp.where(top_in, other, 0.0), pltpu.roll(u, 1, 0))
        down = jnp.where(
            row == rows - 1, jnp.where(bottom_in, other, 0.0), pltpu.roll(u, rows - 1, 0)
        )
        return (up + down) + (pltpu.roll(u, 1, 1) + pltpu.roll(u, lanes - 1, 1))

    def spread(r):
        return jnp.broadcast_to(r, full)

    def explicit_own(h, v, vn):
        inv = inverse(h)

        def body(k, total):
            z = layer(k)
            if h == 0:
                u, other = u_x[z], spread(un_r[k])
            else:
                u = p_s[h - 1, k] * (v + t_s[k])
                other = spread(pr_r[h - 1, k]) * (vn + spread(tr_r[h - 1, k]))
            e = inv * u + pc_x[z] * (beside_own(u, other) - 4.0 * u) + src_x[z]
            total = total + (p_s[h, k] * rl_s[k]) * e
            f_s[k] = total * b_s[h, k]
            return total

        return loop(n, body, jnp.zeros(full, jnp.float32), EXPLICIT)

    def suffix(terms, init, put):
        def block(i, total):
            for c in range(BEHIND // CHUNK):
                first = n - CHUNK * (c + 1) - i * BEHIND
                parts = [terms[first + CHUNK - 1]]
                for j in range(1, CHUNK):
                    parts.append(parts[-1] + terms[first + CHUNK - 1 - j])
                for j, part in enumerate(parts):
                    put(first + CHUNK - 1 - j, total + part)
                total = total + parts[-1]
            return total

        lax.fori_loop(0, n // BEHIND, block, init)

    def behind_own(send):
        def put(k, total):
            t_s[k] = total
            if send:
                tr_s[k] = edge(total)

        suffix(f_s, jnp.zeros(full, jnp.float32), put)

    shifted = lane + 4 * side

    def edge_wait():
        def waiting(slot, ref, sems):
            remote(ref.at[slot], ref.at[slot], e_ss.at[0], sems.at[slot], x_peer).wait_recv()

        def wait_side(s):
            for slot in range(4):
                waiting(slot, en, y_rs)

        for s in range(2):

            @pl.when(at_x[CORE] * at_z[1 - s] == 1)
            def _(s=s):
                for i in range(4 * groups):
                    eo[2 * (1 - s) + CORE, i] = pk[s, i]
                for slot in range(4):
                    if slot != 2 * (1 - s) + CORE:
                        waiting(slot, eo, e_rs)

        when_side(wait_side)

    def far_sends():
        @pl.when(gx == CORE)
        def _():
            pl.semaphore_wait(barrier, 3 + at_z[1] * lefts_there + at_z[0] * rights_there)

        def relay(s):
            for peer in peers:
                tell(far_sem.at[s], peer)

        when_side(relay)
        for q in range(4):
            for s in range(2):
                here = at_z[q // 2] * at_x[q % 2] * there[s]

                @pl.when(here == 1)
                def _(q=q, s=s):
                    if q != 2 * (1 - s) + CORE:
                        pl.semaphore_wait(far_sem.at[s], 1)
                    to_side(s, q).start()

    def edge_unpack():

        filler = lc_x[0]
        zero = jnp.zeros(full, jnp.float32)
        targets = (eu, epc, elc, esrc)

        def unpack(pair, carry):
            for a, e in enumerate(targets):
                rest = filler if a == 2 else zero
                near = [
                    jnp.where(has_side, en[q, a * (groups // 2) + pair], rest) for q in range(4)
                ]
                for s in range(2):
                    g = 2 * pair + s
                    mine = [eo[q, a * groups + g] for q in range(4)]
                    both = {}
                    for m in range(4):
                        x = (shifted - 8 * m - 4 * s) & (lanes - 1)
                        odd = (x // 16) & 1 == 1
                        rel = x & 15
                        from_near = jnp.where(
                            side == 0, (rel < 4).astype(jnp.int32),
                            ((rel >= 8) & (rel < 12)).astype(jnp.int32),
                        ) == 1
                        for rg in range(2):
                            o = jnp.where(odd, mine[2 + rg], mine[rg])
                            w = jnp.where(odd, near[2 + rg], near[rg])
                            both[m, rg] = jnp.where(from_near, w, o)
                    for j in range(SLOTS):
                        x = (shifted - 8 * j - 4 * s) & (lanes - 1)
                        v = jnp.where(x >= 64, both[j % 4, 1], both[j % 4, 0])
                        e[g * SLOTS + j] = pltpu.roll(v, (lanes - 8 * j - 4 * s) % lanes, 1)
            return carry

        lax.fori_loop(0, groups // 2, unpack, 0)

    x_at = shifted & (lanes - 1)
    far_rows, far_layers = x_at >= 64, (x_at // 16) & 1 == 1
    top, bottom = row == 0, row == rows - 1
    across = (top & far_rows) | (bottom & ~far_rows)

    def other_half(a):
        return jnp.where(far_layers, pltpu.roll(a, 16, 1), pltpu.roll(a, lanes - 16, 1))

    def edge_factor():
        ends = factor(lambda k: elc[k], ep, eb, erl, list(range(half)), True)
        for h, (iq, beta) in enumerate(ends):
            eiq[h] = iq
            ebeta[h] = beta

    def edge_step(h):
        inv = inverse(h)

        def explicit(k, total):
            u = eu[k]
            up, down = pltpu.roll(u, 1, 0), pltpu.roll(u, rows - 1, 0)
            over = pltpu.roll(jnp.where(top, up, down), 64, 1)
            over = jnp.where(across, over, 0.0)
            up, down = jnp.where(top, over, up), jnp.where(bottom, over, down)
            beside = (up + down) + (pltpu.roll(u, 1, 1) + pltpu.roll(u, lanes - 1, 1))
            e = inv * u + epc[k] * (beside - 4.0 * u) + esrc[k]
            total = total + (ep[h, k] * erl[k]) * e
            ef[k] = total * eb[h, k]
            return total

        total = loop(n, explicit, jnp.zeros(full, jnp.float32), EXPLICIT)
        iq, beta = eiq[h], ebeta[h]
        face = total * iq
        v = meet(face, beta, iq, other_half(face), other_half(beta))

        def put(k, total):
            eu[k] = ep[h, k] * total

        suffix(ef, v, put)

    def edge_give():
        def give(g, carry):
            moved = [pltpu.roll(eu[g * SLOTS + j], 8 * j, 1) for j in range(SLOTS)]
            for q in range(4):
                b = 16 * (q // 2) + 64 * (q % 2)
                at = ((lane - b) & (lanes - 1)) // WIDTH
                ret_s[q, g] = pltpu.roll(tree(moved, at), (lanes - b) % lanes, 1)
            return carry

        lax.fori_loop(0, groups, give, 0)
        for s in range(2):

            @pl.when(gz == 1 - s)
            def _(s=s):
                for q in range(4):
                    if q != 2 * (1 - s) + CORE:
                        remote(
                            ret_s.at[q], ret_r.at[s], ret_ss.at[q], ret_rs.at[s],
                            (q // 2, q % 2, gy),
                        ).start()
                for g in range(groups):
                    ret_r[s, g] = ret_s[2 * (1 - s) + CORE, g]

    un.wait()
    v = vn = None
    faces = []
    tails = []
    for h in range(half):
        total = explicit_own(h, v, vn)
        face = total * iq_s[h]
        face_s[h] = face
        sends = []
        for s, peer in enumerate(peers):
            if s == 0 or h < last:
                c = remote(face_s.at[h], face_r.at[h, s], fa_ss.at[3 * h + s], fa_rs.at[3 * h + s], peer)
                c.start()
                sends.append(c)
        faces.append(sends)
        if h == 0:
            far_sends()
        if h == 0:
            hs = list(range(1, half))
            for i, (iq, beta) in zip(hs, factor(None, p_s, b_s, rl_s, hs, False, pr_s)):
                iq_s[i] = iq
                beta_s[i] = beta
        behind_own(h < last)
        if h < last:
            c = remote(tr_s, tr_r.at[h], tr_ss.at[h], tr_rs.at[h], x_peer)
            c.start()
            tails.append(c)
        if h == 0:
            for i in hs:
                send_betas(i)
        if h == EDGE_AT:
            edge_wait()

            @pl.when(owner)
            def _():
                edge_unpack()
                edge_factor()
                for i in range(EDGE_SPLIT):
                    edge_step(i)

        if h == EDGE_AT:

            @pl.when(owner)
            def _():
                for i in range(EDGE_SPLIT, half):
                    edge_step(i)
                edge_give()

        for c in betas[h]:
            c.wait()
        if h < last:
            tails[h].wait()
        for c in sends:
            c.wait()
        iq, beta = iq_s[h], beta_s[h]
        v = meet(face_s[h], beta, iq, face_r[h, 0], beta_r[h, 0])
        if h < last:
            w = meet(face_r[h, 1], beta_r[h, 1], iq_r[h], face_r[h, 2], beta_r[h, 2])
            vn = jnp.where(is_low, spread(w[0:1]), spread(w[rows - 1:rows]))

    for s in range(2):

        @pl.when(me != 2 * (1 - s) + CORE)
        def _(s=s):
            remote(
                ret_s.at[0], ret_r.at[s], ret_ss.at[0], ret_rs.at[s], x_peer
            ).wait_recv()

    outer = (lane < 4) | (lane >= lanes - 4)

    def write(g, carry):
        both = jnp.where(low, ret_r[1, g], ret_r[0, g])
        for j in range(SLOTS):
            k = g * SLOTS + j
            u = p_s[last, k] * (v + t_s[k])
            out[layer(k)] = jnp.where(outer, pltpu.roll(both, (lanes - 4 - 8 * j) % lanes, 1), u)
        return carry

    lax.fori_loop(0, groups, write, 0)

    @pl.when(has_left)
    def _():
        to_side(0, 0).wait_send()

    @pl.when(has_right)
    def _():
        to_side(1, 0).wait_send()

    for s in range(2):

        @pl.when(me != 2 * (1 - s) + CORE)
        def _(s=s):
            to_owner(s, 0).wait_send()

    @pl.when(owner)
    def _():
        for q in range(4):

            @pl.when(me != q)
            def _(q=q):
                remote(
                    ret_s.at[q], ret_r.at[0], ret_ss.at[q], ret_rs.at[0], x_peer
                ).wait_send()


def solution(mesh):
    ny_parts = mesh.shape["gy"]
    assert mesh.shape["gz"] == 2 and mesh.shape["gx"] == 2

    def on_device(u, pc, lc, src, table, index):
        half = index.shape[0]
        n, rows, lanes = u.shape
        groups = n // SLOTS
        assert (rows, lanes, half) == (8, 128, 4) and n % (2 * SLOTS) == 0

        def vmem(*dims):
            return pltpu.VMEM(dims, jnp.float32)

        def tiles(*dims):
            return vmem(*dims, rows, lanes)

        dma = pltpu.SemaphoreType.DMA
        scratch = [tiles(n)] * 5 + [tiles(half, n)] * 2 + [tiles(n)] * 2
        scratch += [vmem(n, 1, lanes), vmem(n, 1, lanes), vmem(half - 1, n, 1, lanes)]
        scratch += [vmem(n, 1, lanes), vmem(half - 1, n, 1, lanes), vmem(half - 1, n, 1, lanes)]
        scratch += [tiles(half), tiles(half, 3), tiles(half), tiles(half - 1)]
        scratch += [tiles(half), tiles(half, 3)]
        scratch += [tiles(2, 4 * groups), tiles(2, 2 * groups), tiles(4, 4 * groups), tiles(4, 2 * groups)]
        scratch += [tiles(n)] * 5 + [tiles(half, n)] * 2 + [tiles(n)] + [tiles(half)] * 2
        scratch += [tiles(4, groups), tiles(2, groups)]
        scratch += [dma((4,)), dma((2,))]
        scratch += [dma((half - 1,))] * 4
        scratch += [dma((3 * half,))] * 2
        scratch += [dma((half - 1,))] * 2
        scratch += [dma((3 * half,))] * 2
        scratch += [pltpu.SemaphoreType.REGULAR, pltpu.SemaphoreType.REGULAR((2,))]
        scratch += [dma((2,)), dma((4,)), dma((2,)), dma((4,)), dma((4,)), dma((2,))]
        return pl.pallas_call(
            functools.partial(kernel, ny_parts, half),
            out_shape=pltpu.VMEM(u.shape, jnp.float32),
            in_specs=[pl.BlockSpec(memory_space=pl.ANY)] * 4
            + [pl.BlockSpec(memory_space=pltpu.SMEM)] * 2,
            out_specs=pl.BlockSpec(memory_space=pltpu.VMEM),
            scratch_shapes=scratch,
            compiler_params=pltpu.CompilerParams(collective_id=0, has_side_effects=True),
        )(u, pc, lc, src, table, index)

    spec = P("gz", "gx", "gy")
    return jax.shard_map(
        on_device, mesh=mesh, in_specs=(spec,) * 4 + (P(), P()), out_specs=spec, check_vma=False
    )
```

```python
import functools

import jax
import jax.numpy as jnp
from jax import lax
from jax.experimental import pallas as pl
from jax.experimental.pallas import tpu as pltpu
from jax.sharding import PartitionSpec as P


CORE = 1
EDGE_AT = 2
EDGE_SPLIT = 4
EXPLICIT = 64
BEHIND = 64
CHUNK = 8
FACTOR = 64
SLOTS = 16
WIDTH = 8


def loop(count, body, init, unroll, reverse=False):
    while count % unroll:
        unroll -= 1

    def block(i, carry):
        for j in range(unroll):
            k = i * unroll + j
            carry = body(count - 1 - k if reverse else k, carry)
        return carry

    return lax.fori_loop(0, count // unroll, block, init)


def tree(items, slot):
    bit = 0
    while len(items) > 1:
        odd = (slot >> bit) & 1 == 1
        items = [jnp.where(odd, b, a) for a, b in zip(items[::2], items[1::2])]
        bit += 1
    return items[0]


def kernel(
    ny_parts, half,
    u_in, pc_in, lc_in, src_in, table, index,
    out,
    u_x, pc_x, lc_x, src_x, rl_s, p_s, b_s, f_s, t_s,
    un_s, tr_s, pr_s, un_r, tr_r, pr_r, beta_s, beta_r, iq_s, iq_r, face_s, face_r,
    pk, yk, eo, en, eu, epc, elc, esrc, erl, ep, eb, ef, eiq, ebeta, ret_s, ret_r,
    in_sem, un_sem, tr_ss, tr_rs, pr_ss, pr_rs, be_ss, be_rs, iq_ss, iq_rs, fa_ss, fa_rs,
    group_sem, far_sem, y_ss, y_rs, e_ss, e_rs, ret_ss, ret_rs,
):
    n, rows, lanes = u_in.shape
    last = half - 1
    groups = n // SLOTS
    gz, gx, gy = lax.axis_index("gz"), lax.axis_index("gx"), lax.axis_index("gy")
    has_left, has_right = gy > 0, gy < ny_parts - 1
    owner = gx == CORE
    lefts_there = (gy + ny_parts - 1) // ny_parts
    rights_there = (2 * ny_parts - 2 - gy) // ny_parts
    there = (lefts_there, rights_there)
    sides = (lax.rem(gy + ny_parts - 1, ny_parts), lax.rem(gy + 1, ny_parts))
    at_z, at_x = (1 - gz, gz), (1 - gx, gx)
    side = 1 - gz
    has_side = at_z[1] * lefts_there + at_z[0] * rights_there == 1
    me = 2 * gz + gx
    full = (rows, lanes)

    loads = [
        pltpu.make_async_copy(i, x, in_sem.at[a])
        for a, (i, x) in enumerate(((u_in, u_x), (pc_in, pc_x), (lc_in, lc_x), (src_in, src_x)))
    ]
    for a in (2, 0, 1, 3):
        loads[a].start()

    barrier = pltpu.get_barrier_semaphore()

    def greet(device):
        pl.semaphore_signal(
            barrier, inc=1, device_id=device, device_id_type=pl.DeviceIdType.MESH
        )

    z_peer, x_peer, d_peer = (1 - gz, gx, gy), (gz, 1 - gx, gy), (1 - gz, 1 - gx, gy)
    peers = (z_peer, x_peer, d_peer)
    for peer in peers:
        greet(peer)

    def when_side(act):
        for s in range(2):

            @pl.when(at_x[CORE] * at_z[1 - s] * there[s] == 1)
            def _(s=s):
                act(s)

    def greet_far(s):
        for z in range(2):
            greet((z, CORE, sides[s]))

    when_side(greet_far)

    def remote(src, dst, send, recv, device):
        return pltpu.make_async_remote_copy(
            src_ref=src, dst_ref=dst, send_sem=send, recv_sem=recv,
            device_id=device, device_id_type=pl.DeviceIdType.MESH,
        )

    def layer(k):
        return k + gz * (n - 1 - 2 * k)

    def shift(h):
        return table[index[h]]

    def inverse(h):
        return 1.0 / jnp.full(full, shift(h), jnp.float32)

    lane = lax.broadcasted_iota(jnp.int32, full, 1)
    row = lax.broadcasted_iota(jnp.int32, full, 0)

    is_low = gx == 0

    def edge(x):
        return jnp.where(is_low, x[rows - 1:rows], x[0:1])

    def factor(coupling, p_ref, b_ref, rl_ref, hs, make, row_ref=None):
        inv = [inverse(h) for h in hs]
        one = jnp.ones(full, jnp.float32)

        def body(k, carry):
            if make:
                rl = 1.0 / coupling(k)
                rl_ref[k] = rl
            else:
                rl = rl_ref[k]
            done = []
            for (p, d), h, i in zip(carry, hs, inv):
                add = (rl * i) * p
                q = (p + d) + add
                d = d + add
                p_ref[h, k] = p
                if row_ref is not None and h < last:
                    row_ref[h, k] = edge(p)
                b_ref[h, k] = 1.0 / (p * q)
                done.append((q, d))
            return tuple(done)

        final = loop(n, body, tuple((one, one) for _ in hs), FACTOR)
        ends = []
        for q, d in final:
            iq = 1.0 / q
            ends.append((iq, d * iq))
        return ends

    def meet(face, beta, iq, face_n, beta_n):
        gain = iq / (beta + beta_n - beta * beta_n)
        return (face_n + (1.0 - beta_n) * face) * gain

    loads[2].wait()
    ends = factor(lambda k: lc_x[layer(k)], p_s, b_s, rl_s, [0], True, pr_s)
    iqs = [e[0] for e in ends]
    iq_s[0] = ends[0][0]
    beta_s[0] = ends[0][1]

    for a in (0, 1, 3):
        loads[a].wait()

    base = 16 * gz + 64 * gx
    low = lane % WIDTH < WIDTH // 2
    fields = (u_x, pc_x, lc_x, src_x)

    def pack(pair, carry):
        for a, e in enumerate(fields):
            packed = []
            for s in range(2):
                g = 2 * pair + s
                moved = []
                for j in range(SLOTS):
                    x = e[layer(g * SLOTS + j)]
                    if a == 0:
                        un_s[g * SLOTS + j] = edge(x)
                    moved.append(pltpu.roll(x, (4 + 8 * j + 4 * s) % lanes, 1))
                at_left = ((lane - 4 - 4 * s) & (lanes - 1)) // WIDTH
                at_right = ((lane + 4 - 4 * s) & (lanes - 1)) // WIDTH
                l = pltpu.roll(tree(moved, at_left), base, 1)
                r = pltpu.roll(tree(moved, at_right), base, 1)
                pk[0, a * groups + g] = l
                pk[1, a * groups + g] = r
                packed.append((l, r))
            (l0, r0), (l1, r1) = packed
            yk[0, a * (groups // 2) + pair] = jnp.where(low, l1, l0)
            yk[1, a * (groups // 2) + pair] = jnp.where(low, r0, r1)
        return carry

    for i in range(groups // 2):
        pack(i, 0)

    def tell(sem, device):
        pl.semaphore_signal(sem, inc=1, device_id=device, device_id_type=pl.DeviceIdType.MESH)

    @pl.when(gx != CORE)
    def _():
        pl.semaphore_wait(barrier, 3)
        tell(group_sem, x_peer)

    @pl.when(gx == CORE)
    def _():
        pl.semaphore_wait(group_sem, 1)

    def to_side(s, q):
        return remote(yk.at[s], en.at[q], y_ss.at[s], y_rs.at[q], (s, CORE, sides[s]))

    un = remote(un_s, un_r, un_sem.at[0], un_sem.at[1], x_peer)
    un.start()

    def send_betas(h):
        for s, peer in enumerate(peers):
            if s == 0 or h < last:
                c = remote(beta_s.at[h], beta_r.at[h, s], be_ss.at[3 * h + s], be_rs.at[3 * h + s], peer)
                c.start()
                betas[h].append(c)
        if h < last:
            c = remote(iq_s.at[h], iq_r.at[h], iq_ss.at[h], iq_rs.at[h], x_peer)
            c.start()
            betas[h].append(c)
            c = remote(pr_s.at[h], pr_r.at[h], pr_ss.at[h], pr_rs.at[h], x_peer)
            c.start()
            betas[h].append(c)

    betas = [[] for _ in range(half)]
    send_betas(0)

    def to_owner(s, q):
        return remote(pk.at[s], eo.at[q], e_ss.at[s], e_rs.at[q], (1 - s, CORE, gy))

    for q in range(4):
        for s in range(2):
            if q != 2 * (1 - s) + CORE:

                @pl.when(me == q)
                def _(s=s, q=q):
                    to_owner(s, q).start()

    top_in, bottom_in = gx == 1, gx == 0

    def beside_own(u, other):
        up = jnp.where(row == 0, jnp.where(top_in, other, 0.0), pltpu.roll(u, 1, 0))
        down = jnp.where(
            row == rows - 1, jnp.where(bottom_in, other, 0.0), pltpu.roll(u, rows - 1, 0)
        )
        return (up + down) + (pltpu.roll(u, 1, 1) + pltpu.roll(u, lanes - 1, 1))

    def spread(r):
        return jnp.broadcast_to(r, full)

    def explicit_own(h, v, vn):
        inv = inverse(h)

        def body(k, total):
            z = layer(k)
            if h == 0:
                u, other = u_x[z], spread(un_r[k])
            else:
                u = p_s[h - 1, k] * (v + t_s[k])
                other = spread(pr_r[h - 1, k]) * (vn + spread(tr_r[h - 1, k]))
            e = inv * u + pc_x[z] * (beside_own(u, other) - 4.0 * u) + src_x[z]
            total = total + (p_s[h, k] * rl_s[k]) * e
            f_s[k] = total * b_s[h, k]
            return total

        return loop(n, body, jnp.zeros(full, jnp.float32), EXPLICIT)

    def suffix(terms, init, put):
        def block(i, total):
            for c in range(BEHIND // CHUNK):
                first = n - CHUNK * (c + 1) - i * BEHIND
                parts = [terms[first + CHUNK - 1]]
                for j in range(1, CHUNK):
                    parts.append(parts[-1] + terms[first + CHUNK - 1 - j])
                for j, part in enumerate(parts):
                    put(first + CHUNK - 1 - j, total + part)
                total = total + parts[-1]
            return total

        lax.fori_loop(0, n // BEHIND, block, init)

    def behind_own(send):
        def put(k, total):
            t_s[k] = total
            if send:
                tr_s[k] = edge(total)

        suffix(f_s, jnp.zeros(full, jnp.float32), put)

    shifted = lane + 4 * side

    def edge_wait():
        def waiting(slot, ref, sems):
            remote(ref.at[slot], ref.at[slot], e_ss.at[0], sems.at[slot], x_peer).wait_recv()

        def wait_side(s):
            for slot in range(4):
                waiting(slot, en, y_rs)

        for s in range(2):

            @pl.when(at_x[CORE] * at_z[1 - s] == 1)
            def _(s=s):
                for i in range(4 * groups):
                    eo[2 * (1 - s) + CORE, i] = pk[s, i]
                for slot in range(4):
                    if slot != 2 * (1 - s) + CORE:
                        waiting(slot, eo, e_rs)

        when_side(wait_side)

    def far_sends():
        @pl.when(gx == CORE)
        def _():
            pl.semaphore_wait(barrier, 3 + lefts_there + rights_there)
            tell(far_sem, x_peer)

        @pl.when(gx != CORE)
        def _():
            pl.semaphore_wait(far_sem, 1)

        for q in range(4):
            for s in range(2):
                here = at_z[q // 2] * at_x[q % 2] * there[s]

                @pl.when(here == 1)
                def _(q=q, s=s):
                    to_side(s, q).start()

    def edge_unpack():

        filler = lc_x[0]
        zero = jnp.zeros(full, jnp.float32)
        targets = (eu, epc, elc, esrc)

        def unpack(pair, carry):
            for a, e in enumerate(targets):
                rest = filler if a == 2 else zero
                near = [
                    jnp.where(has_side, en[q, a * (groups // 2) + pair], rest) for q in range(4)
                ]
                for s in range(2):
                    g = 2 * pair + s
                    mine = [eo[q, a * groups + g] for q in range(4)]
                    both = {}
                    for m in range(4):
                        x = (shifted - 8 * m - 4 * s) & (lanes - 1)
                        odd = (x // 16) & 1 == 1
                        rel = x & 15
                        from_near = jnp.where(
                            side == 0, (rel < 4).astype(jnp.int32),
                            ((rel >= 8) & (rel < 12)).astype(jnp.int32),
                        ) == 1
                        for rg in range(2):
                            o = jnp.where(odd, mine[2 + rg], mine[rg])
                            w = jnp.where(odd, near[2 + rg], near[rg])
                            both[m, rg] = jnp.where(from_near, w, o)
                    for j in range(SLOTS):
                        x = (shifted - 8 * j - 4 * s) & (lanes - 1)
                        v = jnp.where(x >= 64, both[j % 4, 1], both[j % 4, 0])
                        e[g * SLOTS + j] = pltpu.roll(v, (lanes - 8 * j - 4 * s) % lanes, 1)
            return carry

        for i in range(groups // 2):
            unpack(i, 0)

    x_at = shifted & (lanes - 1)
    far_rows, far_layers = x_at >= 64, (x_at // 16) & 1 == 1
    top, bottom = row == 0, row == rows - 1
    across = (top & far_rows) | (bottom & ~far_rows)

    def other_half(a):
        return jnp.where(far_layers, pltpu.roll(a, 16, 1), pltpu.roll(a, lanes - 16, 1))

    def edge_factor():
        ends = factor(lambda k: elc[k], ep, eb, erl, list(range(half)), True)
        for h, (iq, beta) in enumerate(ends):
            eiq[h] = iq
            ebeta[h] = beta

    def edge_step(h):
        inv = inverse(h)

        def explicit(k, total):
            u = eu[k]
            up, down = pltpu.roll(u, 1, 0), pltpu.roll(u, rows - 1, 0)
            over = pltpu.roll(jnp.where(top, up, down), 64, 1)
            over = jnp.where(across, over, 0.0)
            up, down = jnp.where(top, over, up), jnp.where(bottom, over, down)
            beside = (up + down) + (pltpu.roll(u, 1, 1) + pltpu.roll(u, lanes - 1, 1))
            e = inv * u + epc[k] * (beside - 4.0 * u) + esrc[k]
            total = total + (ep[h, k] * erl[k]) * e
            ef[k] = total * eb[h, k]
            return total

        total = loop(n, explicit, jnp.zeros(full, jnp.float32), EXPLICIT)
        iq, beta = eiq[h], ebeta[h]
        face = total * iq
        v = meet(face, beta, iq, other_half(face), other_half(beta))

        def put(k, total):
            eu[k] = ep[h, k] * total

        suffix(ef, v, put)

    def edge_give():
        def give(g, carry):
            moved = [pltpu.roll(eu[g * SLOTS + j], 8 * j, 1) for j in range(SLOTS)]
            for q in range(4):
                b = 16 * (q // 2) + 64 * (q % 2)
                at = ((lane - b) & (lanes - 1)) // WIDTH
                ret_s[q, g] = pltpu.roll(tree(moved, at), (lanes - b) % lanes, 1)
            return carry

        for i in range(groups):
            give(i, 0)
        for s in range(2):

            @pl.when(gz == 1 - s)
            def _(s=s):
                for q in range(4):
                    if q != 2 * (1 - s) + CORE:
                        remote(
                            ret_s.at[q], ret_r.at[s], ret_ss.at[q], ret_rs.at[s],
                            (q // 2, q % 2, gy),
                        ).start()
                for g in range(groups):
                    ret_r[s, g] = ret_s[2 * (1 - s) + CORE, g]

    un.wait()
    v = vn = None
    faces = []
    tails = []
    for h in range(half):
        total = explicit_own(h, v, vn)
        face = total * iq_s[h]
        face_s[h] = face
        sends = []
        for s, peer in enumerate(peers):
            if s == 0 or h < last:
                c = remote(face_s.at[h], face_r.at[h, s], fa_ss.at[3 * h + s], fa_rs.at[3 * h + s], peer)
                c.start()
                sends.append(c)
        faces.append(sends)
        if h == 0:
            far_sends()
        if h == 0:
            hs = list(range(1, half))
            for i, (iq, beta) in zip(hs, factor(None, p_s, b_s, rl_s, hs, False, pr_s)):
                iq_s[i] = iq
                beta_s[i] = beta
        behind_own(h < last)
        if h < last:
            c = remote(tr_s, tr_r.at[h], tr_ss.at[h], tr_rs.at[h], x_peer)
            c.start()
            tails.append(c)
        if h == 0:
            for i in hs:
                send_betas(i)
        if h == EDGE_AT:
            edge_wait()

            @pl.when(owner)
            def _():
                edge_unpack()
                edge_factor()
                for i in range(EDGE_SPLIT):
                    edge_step(i)

        if h == EDGE_AT:

            @pl.when(owner)
            def _():
                for i in range(EDGE_SPLIT, half):
                    edge_step(i)
                edge_give()

        for c in betas[h]:
            c.wait()
        if h < last:
            tails[h].wait()
        for c in sends:
            c.wait()
        iq, beta = iq_s[h], beta_s[h]
        v = meet(face_s[h], beta, iq, face_r[h, 0], beta_r[h, 0])
        if h < last:
            w = meet(face_r[h, 1], beta_r[h, 1], iq_r[h], face_r[h, 2], beta_r[h, 2])
            vn = jnp.where(is_low, spread(w[0:1]), spread(w[rows - 1:rows]))

    for s in range(2):

        @pl.when(me != 2 * (1 - s) + CORE)
        def _(s=s):
            remote(
                ret_s.at[0], ret_r.at[s], ret_ss.at[0], ret_rs.at[s], x_peer
            ).wait_recv()

    outer = (lane < 4) | (lane >= lanes - 4)

    def write(g, carry):
        both = jnp.where(low, ret_r[1, g], ret_r[0, g])
        for j in range(SLOTS):
            k = g * SLOTS + j
            u = p_s[last, k] * (v + t_s[k])
            out[layer(k)] = jnp.where(outer, pltpu.roll(both, (lanes - 4 - 8 * j) % lanes, 1), u)
        return carry

    for i in range(groups):
        write(i, 0)

    @pl.when(has_left)
    def _():
        to_side(0, 0).wait_send()

    @pl.when(has_right)
    def _():
        to_side(1, 0).wait_send()

    for s in range(2):

        @pl.when(me != 2 * (1 - s) + CORE)
        def _(s=s):
            to_owner(s, 0).wait_send()

    @pl.when(owner)
    def _():
        for q in range(4):

            @pl.when(me != q)
            def _(q=q):
                remote(
                    ret_s.at[q], ret_r.at[0], ret_ss.at[q], ret_rs.at[0], x_peer
                ).wait_send()


def solution(mesh):
    ny_parts = mesh.shape["gy"]
    assert mesh.shape["gz"] == 2 and mesh.shape["gx"] == 2

    def on_device(u, pc, lc, src, table, index):
        half = index.shape[0]
        n, rows, lanes = u.shape
        groups = n // SLOTS
        assert (rows, lanes, half) == (8, 128, 4) and n % (2 * SLOTS) == 0

        def vmem(*dims):
            return pltpu.VMEM(dims, jnp.float32)

        def tiles(*dims):
            return vmem(*dims, rows, lanes)

        dma = pltpu.SemaphoreType.DMA
        scratch = [tiles(n)] * 5 + [tiles(half, n)] * 2 + [tiles(n)] * 2
        scratch += [vmem(n, 1, lanes), vmem(n, 1, lanes), vmem(half - 1, n, 1, lanes)]
        scratch += [vmem(n, 1, lanes), vmem(half - 1, n, 1, lanes), vmem(half - 1, n, 1, lanes)]
        scratch += [tiles(half), tiles(half, 3), tiles(half), tiles(half - 1)]
        scratch += [tiles(half), tiles(half, 3)]
        scratch += [tiles(2, 4 * groups), tiles(2, 2 * groups), tiles(4, 4 * groups), tiles(4, 2 * groups)]
        scratch += [tiles(n)] * 5 + [tiles(half, n)] * 2 + [tiles(n)] + [tiles(half)] * 2
        scratch += [tiles(4, groups), tiles(2, groups)]
        scratch += [dma((4,)), dma((2,))]
        scratch += [dma((half - 1,))] * 4
        scratch += [dma((3 * half,))] * 2
        scratch += [dma((half - 1,))] * 2
        scratch += [dma((3 * half,))] * 2
        scratch += [pltpu.SemaphoreType.REGULAR] * 2
        scratch += [dma((2,)), dma((4,)), dma((2,)), dma((4,)), dma((4,)), dma((2,))]
        return pl.pallas_call(
            functools.partial(kernel, ny_parts, half),
            out_shape=pltpu.VMEM(u.shape, jnp.float32),
            in_specs=[pl.BlockSpec(memory_space=pl.ANY)] * 4
            + [pl.BlockSpec(memory_space=pltpu.SMEM)] * 2,
            out_specs=pl.BlockSpec(memory_space=pltpu.VMEM),
            scratch_shapes=scratch,
            compiler_params=pltpu.CompilerParams(collective_id=0, has_side_effects=True),
        )(u, pc, lc, src, table, index)

    spec = P("gz", "gx", "gy")
    return jax.shard_map(
        on_device, mesh=mesh, in_specs=(spec,) * 4 + (P(), P()), out_specs=spec, check_vma=False
    )
```

```python
import functools

import jax
import jax.numpy as jnp
from jax import lax
from jax.experimental import pallas as pl
from jax.experimental.pallas import tpu as pltpu
from jax.sharding import PartitionSpec as P


CORE = 1
EDGE_AT = 2
EDGE_SPLIT = 4
EXPLICIT = 64
BEHIND = 64
CHUNK = 8
FACTOR = 64
SLOTS = 16
WIDTH = 8


def loop(count, body, init, unroll, reverse=False):
    while count % unroll:
        unroll -= 1

    def block(i, carry):
        for j in range(unroll):
            k = i * unroll + j
            carry = body(count - 1 - k if reverse else k, carry)
        return carry

    return lax.fori_loop(0, count // unroll, block, init)


def tree(items, slot):
    bit = 0
    while len(items) > 1:
        odd = (slot >> bit) & 1 == 1
        items = [jnp.where(odd, b, a) for a, b in zip(items[::2], items[1::2])]
        bit += 1
    return items[0]


def kernel(
    ny_parts, half,
    u_in, pc_in, lc_in, src_in, table, index,
    out,
    u_x, pc_x, lc_x, src_x, rl_s, p_s, b_s, f_s, t_s,
    un_s, tr_s, pr_s, un_r, tr_r, pr_r, beta_s, beta_r, iq_s, iq_r, face_s, face_r,
    pk, yk, eo, en, eu, epc, elc, esrc, erl, ep, eb, ef, eiq, ebeta, ret_s, ret_r,
    in_sem, un_sem, tr_ss, tr_rs, pr_ss, pr_rs, be_ss, be_rs, iq_ss, iq_rs, fa_ss, fa_rs,
    group_sem, far_sem, y_ss, y_rs, e_ss, e_rs, ret_ss, ret_rs,
):
    n, rows, lanes = u_in.shape
    last = half - 1
    groups = n // SLOTS
    gz, gx, gy = lax.axis_index("gz"), lax.axis_index("gx"), lax.axis_index("gy")
    has_left, has_right = gy > 0, gy < ny_parts - 1
    owner = gx == CORE
    lefts_there = (gy + ny_parts - 1) // ny_parts
    rights_there = (2 * ny_parts - 2 - gy) // ny_parts
    there = (lefts_there, rights_there)
    sides = (lax.rem(gy + ny_parts - 1, ny_parts), lax.rem(gy + 1, ny_parts))
    at_z, at_x = (1 - gz, gz), (1 - gx, gx)
    side = 1 - gz
    has_side = at_z[1] * lefts_there + at_z[0] * rights_there == 1
    me = 2 * gz + gx
    full = (rows, lanes)

    loads = [
        pltpu.make_async_copy(i, x, in_sem.at[a])
        for a, (i, x) in enumerate(((u_in, u_x), (pc_in, pc_x), (lc_in, lc_x), (src_in, src_x)))
    ]
    for a in (2, 0, 1, 3):
        loads[a].start()

    barrier = pltpu.get_barrier_semaphore()

    def greet(device):
        pl.semaphore_signal(
            barrier, inc=1, device_id=device, device_id_type=pl.DeviceIdType.MESH
        )

    z_peer, x_peer, d_peer = (1 - gz, gx, gy), (gz, 1 - gx, gy), (1 - gz, 1 - gx, gy)
    peers = (z_peer, x_peer, d_peer)
    for peer in peers:
        greet(peer)

    def when_side(act):
        for s in range(2):

            @pl.when(at_x[CORE] * at_z[1 - s] * there[s] == 1)
            def _(s=s):
                act(s)

    def greet_far(s):
        for z in range(2):
            greet((z, CORE, sides[s]))

    when_side(greet_far)

    def remote(src, dst, send, recv, device):
        return pltpu.make_async_remote_copy(
            src_ref=src, dst_ref=dst, send_sem=send, recv_sem=recv,
            device_id=device, device_id_type=pl.DeviceIdType.MESH,
        )

    def layer(k):
        return k + gz * (n - 1 - 2 * k)

    def shift(h):
        return table[index[h]]

    def inverse(h):
        return 1.0 / jnp.full(full, shift(h), jnp.float32)

    lane = lax.broadcasted_iota(jnp.int32, full, 1)
    row = lax.broadcasted_iota(jnp.int32, full, 0)

    is_low = gx == 0

    def edge(x):
        return jnp.where(is_low, x[rows - 1:rows], x[0:1])

    def factor(coupling, p_ref, b_ref, rl_ref, hs, make, row_ref=None):
        inv = [inverse(h) for h in hs]
        one = jnp.ones(full, jnp.float32)

        def body(k, carry):
            if make:
                rl = 1.0 / coupling(k)
                rl_ref[k] = rl
            else:
                rl = rl_ref[k]
            done = []
            for (p, d), h, i in zip(carry, hs, inv):
                add = (rl * i) * p
                q = (p + d) + add
                d = d + add
                p_ref[h, k] = p
                if row_ref is not None and h < last:
                    row_ref[h, k] = edge(p)
                b_ref[h, k] = 1.0 / (p * q)
                done.append((q, d))
            return tuple(done)

        final = loop(n, body, tuple((one, one) for _ in hs), FACTOR)
        ends = []
        for q, d in final:
            iq = 1.0 / q
            ends.append((iq, d * iq))
        return ends

    def meet(face, beta, iq, face_n, beta_n):
        gain = iq / (beta + beta_n - beta * beta_n)
        return (face_n + (1.0 - beta_n) * face) * gain

    loads[2].wait()
    ends = factor(lambda k: lc_x[layer(k)], p_s, b_s, rl_s, [0], True, pr_s)
    iqs = [e[0] for e in ends]
    iq_s[0] = ends[0][0]
    beta_s[0] = ends[0][1]

    loads[0].wait()
    for k in range(n):
        un_s[k] = edge(u_x[layer(k)])

    base = 16 * gz + 64 * gx
    low = lane % WIDTH < WIDTH // 2
    fields = (u_x, pc_x, lc_x, src_x)

    def pack(pair, carry):
        for a, e in enumerate(fields):
            packed = []
            for s in range(2):
                g = 2 * pair + s
                moved = []
                for j in range(SLOTS):
                    x = e[layer(g * SLOTS + j)]
                    moved.append(pltpu.roll(x, (4 + 8 * j + 4 * s) % lanes, 1))
                at_left = ((lane - 4 - 4 * s) & (lanes - 1)) // WIDTH
                at_right = ((lane + 4 - 4 * s) & (lanes - 1)) // WIDTH
                l = pltpu.roll(tree(moved, at_left), base, 1)
                r = pltpu.roll(tree(moved, at_right), base, 1)
                pk[0, a * groups + g] = l
                pk[1, a * groups + g] = r
                packed.append((l, r))
            (l0, r0), (l1, r1) = packed
            yk[0, a * (groups // 2) + pair] = jnp.where(low, l1, l0)
            yk[1, a * (groups // 2) + pair] = jnp.where(low, r0, r1)
        return carry


    def tell(sem, device):
        pl.semaphore_signal(sem, inc=1, device_id=device, device_id_type=pl.DeviceIdType.MESH)

    @pl.when(gx != CORE)
    def _():
        pl.semaphore_wait(barrier, 3)
        tell(group_sem, x_peer)

    @pl.when(gx == CORE)
    def _():
        pl.semaphore_wait(group_sem, 1)

    def to_side(s, q):
        return remote(yk.at[s], en.at[q], y_ss.at[s], y_rs.at[q], (s, CORE, sides[s]))

    un = remote(un_s, un_r, un_sem.at[0], un_sem.at[1], x_peer)
    un.start()

    def send_betas(h):
        for s, peer in enumerate(peers):
            if s == 0 or h < last:
                c = remote(beta_s.at[h], beta_r.at[h, s], be_ss.at[3 * h + s], be_rs.at[3 * h + s], peer)
                c.start()
                betas[h].append(c)
        if h < last:
            c = remote(iq_s.at[h], iq_r.at[h], iq_ss.at[h], iq_rs.at[h], x_peer)
            c.start()
            betas[h].append(c)
            c = remote(pr_s.at[h], pr_r.at[h], pr_ss.at[h], pr_rs.at[h], x_peer)
            c.start()
            betas[h].append(c)

    betas = [[] for _ in range(half)]
    send_betas(0)

    def to_owner(s, q):
        return remote(pk.at[s], eo.at[q], e_ss.at[s], e_rs.at[q], (1 - s, CORE, gy))

    top_in, bottom_in = gx == 1, gx == 0

    def beside_own(u, other):
        up = jnp.where(row == 0, jnp.where(top_in, other, 0.0), pltpu.roll(u, 1, 0))
        down = jnp.where(
            row == rows - 1, jnp.where(bottom_in, other, 0.0), pltpu.roll(u, rows - 1, 0)
        )
        return (up + down) + (pltpu.roll(u, 1, 1) + pltpu.roll(u, lanes - 1, 1))

    def spread(r):
        return jnp.broadcast_to(r, full)

    def explicit_own(h, v, vn):
        inv = inverse(h)

        def body(k, total):
            z = layer(k)
            if h == 0:
                u, other = u_x[z], spread(un_r[k])
            else:
                u = p_s[h - 1, k] * (v + t_s[k])
                other = spread(pr_r[h - 1, k]) * (vn + spread(tr_r[h - 1, k]))
            e = inv * u + pc_x[z] * (beside_own(u, other) - 4.0 * u) + src_x[z]
            total = total + (p_s[h, k] * rl_s[k]) * e
            f_s[k] = total * b_s[h, k]
            return total

        return loop(n, body, jnp.zeros(full, jnp.float32), EXPLICIT)

    def suffix(terms, init, put):
        def block(i, total):
            for c in range(BEHIND // CHUNK):
                first = n - CHUNK * (c + 1) - i * BEHIND
                parts = [terms[first + CHUNK - 1]]
                for j in range(1, CHUNK):
                    parts.append(parts[-1] + terms[first + CHUNK - 1 - j])
                for j, part in enumerate(parts):
                    put(first + CHUNK - 1 - j, total + part)
                total = total + parts[-1]
            return total

        lax.fori_loop(0, n // BEHIND, block, init)

    def behind_own(send):
        def put(k, total):
            t_s[k] = total
            if send:
                tr_s[k] = edge(total)

        suffix(f_s, jnp.zeros(full, jnp.float32), put)

    shifted = lane + 4 * side

    def edge_wait():
        def waiting(slot, ref, sems):
            remote(ref.at[slot], ref.at[slot], e_ss.at[0], sems.at[slot], x_peer).wait_recv()

        def wait_side(s):
            for slot in range(4):
                waiting(slot, en, y_rs)

        for s in range(2):

            @pl.when(at_x[CORE] * at_z[1 - s] == 1)
            def _(s=s):
                for i in range(4 * groups):
                    eo[2 * (1 - s) + CORE, i] = pk[s, i]
                for slot in range(4):
                    if slot != 2 * (1 - s) + CORE:
                        waiting(slot, eo, e_rs)

        when_side(wait_side)

    def own_sends():
        for q in range(4):
            for s in range(2):
                if q != 2 * (1 - s) + CORE:

                    @pl.when(me == q)
                    def _(s=s, q=q):
                        to_owner(s, q).start()

    def far_sends():
        @pl.when(gx == CORE)
        def _():
            pl.semaphore_wait(barrier, 3 + lefts_there + rights_there)
            tell(far_sem, x_peer)

        @pl.when(gx != CORE)
        def _():
            pl.semaphore_wait(far_sem, 1)

        for q in range(4):
            for s in range(2):
                here = at_z[q // 2] * at_x[q % 2] * there[s]

                @pl.when(here == 1)
                def _(q=q, s=s):
                    to_side(s, q).start()

    def edge_unpack():

        filler = lc_x[0]
        zero = jnp.zeros(full, jnp.float32)
        targets = (eu, epc, elc, esrc)

        def unpack(pair, carry):
            for a, e in enumerate(targets):
                rest = filler if a == 2 else zero
                near = [
                    jnp.where(has_side, en[q, a * (groups // 2) + pair], rest) for q in range(4)
                ]
                for s in range(2):
                    g = 2 * pair + s
                    mine = [eo[q, a * groups + g] for q in range(4)]
                    both = {}
                    for m in range(4):
                        x = (shifted - 8 * m - 4 * s) & (lanes - 1)
                        odd = (x // 16) & 1 == 1
                        rel = x & 15
                        from_near = jnp.where(
                            side == 0, (rel < 4).astype(jnp.int32),
                            ((rel >= 8) & (rel < 12)).astype(jnp.int32),
                        ) == 1
                        for rg in range(2):
                            o = jnp.where(odd, mine[2 + rg], mine[rg])
                            w = jnp.where(odd, near[2 + rg], near[rg])
                            both[m, rg] = jnp.where(from_near, w, o)
                    for j in range(SLOTS):
                        x = (shifted - 8 * j - 4 * s) & (lanes - 1)
                        v = jnp.where(x >= 64, both[j % 4, 1], both[j % 4, 0])
                        e[g * SLOTS + j] = pltpu.roll(v, (lanes - 8 * j - 4 * s) % lanes, 1)
            return carry

        for i in range(groups // 2):
            unpack(i, 0)

    x_at = shifted & (lanes - 1)
    far_rows, far_layers = x_at >= 64, (x_at // 16) & 1 == 1
    top, bottom = row == 0, row == rows - 1
    across = (top & far_rows) | (bottom & ~far_rows)

    def other_half(a):
        return jnp.where(far_layers, pltpu.roll(a, 16, 1), pltpu.roll(a, lanes - 16, 1))

    def edge_factor():
        ends = factor(lambda k: elc[k], ep, eb, erl, list(range(half)), True)
        for h, (iq, beta) in enumerate(ends):
            eiq[h] = iq
            ebeta[h] = beta

    def edge_step(h):
        inv = inverse(h)

        def explicit(k, total):
            u = eu[k]
            up, down = pltpu.roll(u, 1, 0), pltpu.roll(u, rows - 1, 0)
            over = pltpu.roll(jnp.where(top, up, down), 64, 1)
            over = jnp.where(across, over, 0.0)
            up, down = jnp.where(top, over, up), jnp.where(bottom, over, down)
            beside = (up + down) + (pltpu.roll(u, 1, 1) + pltpu.roll(u, lanes - 1, 1))
            e = inv * u + epc[k] * (beside - 4.0 * u) + esrc[k]
            total = total + (ep[h, k] * erl[k]) * e
            ef[k] = total * eb[h, k]
            return total

        total = loop(n, explicit, jnp.zeros(full, jnp.float32), EXPLICIT)
        iq, beta = eiq[h], ebeta[h]
        face = total * iq
        v = meet(face, beta, iq, other_half(face), other_half(beta))

        def put(k, total):
            eu[k] = ep[h, k] * total

        suffix(ef, v, put)

    def edge_give():
        def give(g, carry):
            moved = [pltpu.roll(eu[g * SLOTS + j], 8 * j, 1) for j in range(SLOTS)]
            for q in range(4):
                b = 16 * (q // 2) + 64 * (q % 2)
                at = ((lane - b) & (lanes - 1)) // WIDTH
                ret_s[q, g] = pltpu.roll(tree(moved, at), (lanes - b) % lanes, 1)
            return carry

        for i in range(groups):
            give(i, 0)
        for s in range(2):

            @pl.when(gz == 1 - s)
            def _(s=s):
                for q in range(4):
                    if q != 2 * (1 - s) + CORE:
                        remote(
                            ret_s.at[q], ret_r.at[s], ret_ss.at[q], ret_rs.at[s],
                            (q // 2, q % 2, gy),
                        ).start()
                for g in range(groups):
                    ret_r[s, g] = ret_s[2 * (1 - s) + CORE, g]

    for a in (1, 3):
        loads[a].wait()
    for i in range(groups // 2):
        pack(i, 0)
    un.wait()
    v = vn = None
    faces = []
    tails = []
    for h in range(half):
        total = explicit_own(h, v, vn)
        face = total * iq_s[h]
        face_s[h] = face
        sends = []
        for s, peer in enumerate(peers):
            if s == 0 or h < last:
                c = remote(face_s.at[h], face_r.at[h, s], fa_ss.at[3 * h + s], fa_rs.at[3 * h + s], peer)
                c.start()
                sends.append(c)
        faces.append(sends)
        if h == 0:
            far_sends()
            own_sends()
        if h == 0:
            hs = list(range(1, half))
            for i, (iq, beta) in zip(hs, factor(None, p_s, b_s, rl_s, hs, False, pr_s)):
                iq_s[i] = iq
                beta_s[i] = beta
        behind_own(h < last)
        if h < last:
            c = remote(tr_s, tr_r.at[h], tr_ss.at[h], tr_rs.at[h], x_peer)
            c.start()
            tails.append(c)
        if h == 0:
            for i in hs:
                send_betas(i)
        if h == EDGE_AT:
            edge_wait()

            @pl.when(owner)
            def _():
                edge_unpack()
                edge_factor()
                for i in range(EDGE_SPLIT):
                    edge_step(i)

        if h == EDGE_AT:

            @pl.when(owner)
            def _():
                for i in range(EDGE_SPLIT, half):
                    edge_step(i)
                edge_give()

        for c in betas[h]:
            c.wait()
        if h < last:
            tails[h].wait()
        for c in sends:
            c.wait()
        iq, beta = iq_s[h], beta_s[h]
        v = meet(face_s[h], beta, iq, face_r[h, 0], beta_r[h, 0])
        if h < last:
            w = meet(face_r[h, 1], beta_r[h, 1], iq_r[h], face_r[h, 2], beta_r[h, 2])
            vn = jnp.where(is_low, spread(w[0:1]), spread(w[rows - 1:rows]))

    for s in range(2):

        @pl.when(me != 2 * (1 - s) + CORE)
        def _(s=s):
            remote(
                ret_s.at[0], ret_r.at[s], ret_ss.at[0], ret_rs.at[s], x_peer
            ).wait_recv()

    outer = (lane < 4) | (lane >= lanes - 4)

    def write(g, carry):
        both = jnp.where(low, ret_r[1, g], ret_r[0, g])
        for j in range(SLOTS):
            k = g * SLOTS + j
            u = p_s[last, k] * (v + t_s[k])
            out[layer(k)] = jnp.where(outer, pltpu.roll(both, (lanes - 4 - 8 * j) % lanes, 1), u)
        return carry

    for i in range(groups):
        write(i, 0)

    @pl.when(has_left)
    def _():
        to_side(0, 0).wait_send()

    @pl.when(has_right)
    def _():
        to_side(1, 0).wait_send()

    for s in range(2):

        @pl.when(me != 2 * (1 - s) + CORE)
        def _(s=s):
            to_owner(s, 0).wait_send()

    @pl.when(owner)
    def _():
        for q in range(4):

            @pl.when(me != q)
            def _(q=q):
                remote(
                    ret_s.at[q], ret_r.at[0], ret_ss.at[q], ret_rs.at[0], x_peer
                ).wait_send()


def solution(mesh):
    ny_parts = mesh.shape["gy"]
    assert mesh.shape["gz"] == 2 and mesh.shape["gx"] == 2

    def on_device(u, pc, lc, src, table, index):
        half = index.shape[0]
        n, rows, lanes = u.shape
        groups = n // SLOTS
        assert (rows, lanes, half) == (8, 128, 4) and n % (2 * SLOTS) == 0

        def vmem(*dims):
            return pltpu.VMEM(dims, jnp.float32)

        def tiles(*dims):
            return vmem(*dims, rows, lanes)

        dma = pltpu.SemaphoreType.DMA
        scratch = [tiles(n)] * 5 + [tiles(half, n)] * 2 + [tiles(n)] * 2
        scratch += [vmem(n, 1, lanes), vmem(n, 1, lanes), vmem(half - 1, n, 1, lanes)]
        scratch += [vmem(n, 1, lanes), vmem(half - 1, n, 1, lanes), vmem(half - 1, n, 1, lanes)]
        scratch += [tiles(half), tiles(half, 3), tiles(half), tiles(half - 1)]
        scratch += [tiles(half), tiles(half, 3)]
        scratch += [tiles(2, 4 * groups), tiles(2, 2 * groups), tiles(4, 4 * groups), tiles(4, 2 * groups)]
        scratch += [tiles(n)] * 5 + [tiles(half, n)] * 2 + [tiles(n)] + [tiles(half)] * 2
        scratch += [tiles(4, groups), tiles(2, groups)]
        scratch += [dma((4,)), dma((2,))]
        scratch += [dma((half - 1,))] * 4
        scratch += [dma((3 * half,))] * 2
        scratch += [dma((half - 1,))] * 2
        scratch += [dma((3 * half,))] * 2
        scratch += [pltpu.SemaphoreType.REGULAR] * 2
        scratch += [dma((2,)), dma((4,)), dma((2,)), dma((4,)), dma((4,)), dma((2,))]
        return pl.pallas_call(
            functools.partial(kernel, ny_parts, half),
            out_shape=pltpu.VMEM(u.shape, jnp.float32),
            in_specs=[pl.BlockSpec(memory_space=pl.ANY)] * 4
            + [pl.BlockSpec(memory_space=pltpu.SMEM)] * 2,
            out_specs=pl.BlockSpec(memory_space=pltpu.VMEM),
            scratch_shapes=scratch,
            compiler_params=pltpu.CompilerParams(collective_id=0, has_side_effects=True),
        )(u, pc, lc, src, table, index)

    spec = P("gz", "gx", "gy")
    return jax.shard_map(
        on_device, mesh=mesh, in_specs=(spec,) * 4 + (P(), P()), out_specs=spec, check_vma=False
    )
```

```python
import functools

import jax
import jax.numpy as jnp
from jax import lax
from jax.experimental import pallas as pl
from jax.experimental.pallas import tpu as pltpu
from jax.sharding import PartitionSpec as P


CORE = 1
EDGE_AT = 2
EDGE_SPLIT = 4
EXPLICIT = 64
BEHIND = 64
CHUNK = 8
FACTOR = 64
SLOTS = 16
WIDTH = 8


def loop(count, body, init, unroll, reverse=False):
    while count % unroll:
        unroll -= 1

    def block(i, carry):
        for j in range(unroll):
            k = i * unroll + j
            carry = body(count - 1 - k if reverse else k, carry)
        return carry

    return lax.fori_loop(0, count // unroll, block, init)


def tree(items, slot):
    bit = 0
    while len(items) > 1:
        odd = (slot >> bit) & 1 == 1
        items = [jnp.where(odd, b, a) for a, b in zip(items[::2], items[1::2])]
        bit += 1
    return items[0]


def kernel(
    ny_parts, half,
    u_in, pc_in, lc_in, src_in, table, index,
    out,
    u_x, pc_x, lc_x, src_x, rl_s, p_s, b_s, f_s, t_s,
    un_s, tr_s, pr_s, un_r, tr_r, pr_r, beta_s, beta_r, iq_s, iq_r, face_s, face_r,
    pk, yk, eo, en, eu, epc, elc, esrc, erl, ep, eb, ef, eiq, ebeta, ret_s, ret_r,
    in_sem, un_sem, tr_ss, tr_rs, pr_ss, pr_rs, be_ss, be_rs, iq_ss, iq_rs, fa_ss, fa_rs,
    group_sem, far_sem, y_ss, y_rs, e_ss, e_rs, ret_ss, ret_rs,
):
    n, rows, lanes = u_in.shape
    last = half - 1
    groups = n // SLOTS
    gz, gx, gy = lax.axis_index("gz"), lax.axis_index("gx"), lax.axis_index("gy")
    has_left, has_right = gy > 0, gy < ny_parts - 1
    owner = gx == CORE
    lefts_there = (gy + ny_parts - 1) // ny_parts
    rights_there = (2 * ny_parts - 2 - gy) // ny_parts
    there = (lefts_there, rights_there)
    sides = (lax.rem(gy + ny_parts - 1, ny_parts), lax.rem(gy + 1, ny_parts))
    at_z, at_x = (1 - gz, gz), (1 - gx, gx)
    side = 1 - gz
    has_side = at_z[1] * lefts_there + at_z[0] * rights_there == 1
    me = 2 * gz + gx
    full = (rows, lanes)

    loads = [
        pltpu.make_async_copy(i, x, in_sem.at[a])
        for a, (i, x) in enumerate(((u_in, u_x), (pc_in, pc_x), (lc_in, lc_x), (src_in, src_x)))
    ]
    for a in (2, 0, 1, 3):
        loads[a].start()

    barrier = pltpu.get_barrier_semaphore()

    def greet(device):
        pl.semaphore_signal(
            barrier, inc=1, device_id=device, device_id_type=pl.DeviceIdType.MESH
        )

    z_peer, x_peer, d_peer = (1 - gz, gx, gy), (gz, 1 - gx, gy), (1 - gz, 1 - gx, gy)
    peers = (z_peer, x_peer, d_peer)
    for peer in peers:
        greet(peer)

    def when_side(act):
        for s in range(2):

            @pl.when(at_x[CORE] * at_z[1 - s] * there[s] == 1)
            def _(s=s):
                act(s)

    def greet_far(s):
        for z in range(2):
            greet((z, CORE, sides[s]))

    when_side(greet_far)

    def remote(src, dst, send, recv, device):
        return pltpu.make_async_remote_copy(
            src_ref=src, dst_ref=dst, send_sem=send, recv_sem=recv,
            device_id=device, device_id_type=pl.DeviceIdType.MESH,
        )

    def layer(k):
        return k + gz * (n - 1 - 2 * k)

    def shift(h):
        return table[index[h]]

    def inverse(h):
        return 1.0 / jnp.full(full, shift(h), jnp.float32)

    lane = lax.broadcasted_iota(jnp.int32, full, 1)
    row = lax.broadcasted_iota(jnp.int32, full, 0)

    is_low = gx == 0

    def edge(x):
        return jnp.where(is_low, x[rows - 1:rows], x[0:1])

    def factor(coupling, p_ref, b_ref, rl_ref, hs, make, row_ref=None):
        inv = [inverse(h) for h in hs]
        one = jnp.ones(full, jnp.float32)

        def body(k, carry):
            if make:
                rl = 1.0 / coupling(k)
                rl_ref[k] = rl
            else:
                rl = rl_ref[k]
            done = []
            for (p, d), h, i in zip(carry, hs, inv):
                add = (rl * i) * p
                q = (p + d) + add
                d = d + add
                p_ref[h, k] = p
                if row_ref is not None and h < last:
                    row_ref[h, k] = edge(p)
                b_ref[h, k] = 1.0 / (p * q)
                done.append((q, d))
            return tuple(done)

        final = loop(n, body, tuple((one, one) for _ in hs), FACTOR)
        ends = []
        for q, d in final:
            iq = 1.0 / q
            ends.append((iq, d * iq))
        return ends

    def meet(face, beta, iq, face_n, beta_n):
        gain = iq / (beta + beta_n - beta * beta_n)
        return (face_n + (1.0 - beta_n) * face) * gain

    loads[2].wait()
    ends = factor(lambda k: lc_x[layer(k)], p_s, b_s, rl_s, [0], True, pr_s)
    iqs = [e[0] for e in ends]
    iq_s[0] = ends[0][0]
    beta_s[0] = ends[0][1]

    loads[0].wait()
    for k in range(n):
        un_s[k] = edge(u_x[layer(k)])

    base = 16 * gz + 64 * gx
    low = lane % WIDTH < WIDTH // 2
    fields = (u_x, pc_x, lc_x, src_x)

    def pack(pair, carry):
        for a, e in enumerate(fields):
            packed = []
            for s in range(2):
                g = 2 * pair + s
                moved = []
                for j in range(SLOTS):
                    x = e[layer(g * SLOTS + j)]
                    moved.append(pltpu.roll(x, (4 + 8 * j + 4 * s) % lanes, 1))
                at_left = ((lane - 4 - 4 * s) & (lanes - 1)) // WIDTH
                at_right = ((lane + 4 - 4 * s) & (lanes - 1)) // WIDTH
                l = pltpu.roll(tree(moved, at_left), base, 1)
                r = pltpu.roll(tree(moved, at_right), base, 1)
                pk[0, a * groups + g] = l
                pk[1, a * groups + g] = r
                packed.append((l, r))
            (l0, r0), (l1, r1) = packed
            yk[0, a * (groups // 2) + pair] = jnp.where(low, l1, l0)
            yk[1, a * (groups // 2) + pair] = jnp.where(low, r0, r1)
        return carry


    def tell(sem, device):
        pl.semaphore_signal(sem, inc=1, device_id=device, device_id_type=pl.DeviceIdType.MESH)

    @pl.when(gx != CORE)
    def _():
        pl.semaphore_wait(barrier, 3)
        tell(group_sem, x_peer)

    @pl.when(gx == CORE)
    def _():
        pl.semaphore_wait(group_sem, 1)

    def to_side(s, q):
        return remote(yk.at[s], en.at[q], y_ss.at[s], y_rs.at[q], (s, CORE, sides[s]))

    un = remote(un_s, un_r, un_sem.at[0], un_sem.at[1], x_peer)
    un.start()

    def send_betas(h):
        for s, peer in enumerate(peers):
            if s == 0 or h < last:
                c = remote(beta_s.at[h], beta_r.at[h, s], be_ss.at[3 * h + s], be_rs.at[3 * h + s], peer)
                c.start()
                betas[h].append(c)
        if h < last:
            c = remote(iq_s.at[h], iq_r.at[h], iq_ss.at[h], iq_rs.at[h], x_peer)
            c.start()
            betas[h].append(c)
            c = remote(pr_s.at[h], pr_r.at[h], pr_ss.at[h], pr_rs.at[h], x_peer)
            c.start()
            betas[h].append(c)

    betas = [[] for _ in range(half)]
    send_betas(0)

    def to_owner(s, q):
        return remote(pk.at[s], eo.at[q], e_ss.at[s], e_rs.at[q], (1 - s, CORE, gy))

    top_in, bottom_in = gx == 1, gx == 0

    shared = row == (rows - 1) * gx
    border = row == (rows - 1) * (1 - gx)
    towards = 1 + (rows - 2) * (1 - gx)

    def beside_own(u, other):
        inner = pltpu.roll(jnp.where(shared, other, u), towards, 0)
        outer = pltpu.roll(jnp.where(border, 0.0, u), rows - towards, 0)
        return (inner + outer) + (pltpu.roll(u, 1, 1) + pltpu.roll(u, lanes - 1, 1))

    def spread(r):
        return jnp.broadcast_to(r, full)

    def explicit_own(h, v, vn):
        inv = inverse(h)

        def body(k, total):
            z = layer(k)
            if h == 0:
                u, other = u_x[z], spread(un_r[k])
            else:
                u = p_s[h - 1, k] * (v + t_s[k])
                other = spread(pr_r[h - 1, k]) * (vn + spread(tr_r[h - 1, k]))
            e = inv * u + pc_x[z] * (beside_own(u, other) - 4.0 * u) + src_x[z]
            total = total + (p_s[h, k] * rl_s[k]) * e
            f_s[k] = total * b_s[h, k]
            return total

        return loop(n, body, jnp.zeros(full, jnp.float32), EXPLICIT)

    def suffix(terms, init, put):
        def block(i, total):
            for c in range(BEHIND // CHUNK):
                first = n - CHUNK * (c + 1) - i * BEHIND
                parts = [terms[first + CHUNK - 1]]
                for j in range(1, CHUNK):
                    parts.append(parts[-1] + terms[first + CHUNK - 1 - j])
                for j, part in enumerate(parts):
                    put(first + CHUNK - 1 - j, total + part)
                total = total + parts[-1]
            return total

        lax.fori_loop(0, n // BEHIND, block, init)

    def behind_own(send):
        def put(k, total):
            t_s[k] = total
            if send:
                tr_s[k] = edge(total)

        suffix(f_s, jnp.zeros(full, jnp.float32), put)

    shifted = lane + 4 * side

    def edge_wait():
        def waiting(slot, ref, sems):
            remote(ref.at[slot], ref.at[slot], e_ss.at[0], sems.at[slot], x_peer).wait_recv()

        def wait_side(s):
            for slot in range(4):
                waiting(slot, en, y_rs)

        for s in range(2):

            @pl.when(at_x[CORE] * at_z[1 - s] == 1)
            def _(s=s):
                for i in range(4 * groups):
                    eo[2 * (1 - s) + CORE, i] = pk[s, i]
                for slot in range(4):
                    if slot != 2 * (1 - s) + CORE:
                        waiting(slot, eo, e_rs)

        when_side(wait_side)

    def own_sends():
        for q in range(4):
            for s in range(2):
                if q != 2 * (1 - s) + CORE:

                    @pl.when(me == q)
                    def _(s=s, q=q):
                        to_owner(s, q).start()

    def far_sends():
        @pl.when(gx == CORE)
        def _():
            pl.semaphore_wait(barrier, 3 + lefts_there + rights_there)
            tell(far_sem, x_peer)

        @pl.when(gx != CORE)
        def _():
            pl.semaphore_wait(far_sem, 1)

        for q in range(4):
            for s in range(2):
                here = at_z[q // 2] * at_x[q % 2] * there[s]

                @pl.when(here == 1)
                def _(q=q, s=s):
                    to_side(s, q).start()

    def edge_unpack():

        filler = lc_x[0]
        zero = jnp.zeros(full, jnp.float32)
        targets = (eu, epc, elc, esrc)

        def unpack(pair, carry):
            for a, e in enumerate(targets):
                rest = filler if a == 2 else zero
                near = [
                    jnp.where(has_side, en[q, a * (groups // 2) + pair], rest) for q in range(4)
                ]
                for s in range(2):
                    g = 2 * pair + s
                    mine = [eo[q, a * groups + g] for q in range(4)]
                    both = {}
                    for m in range(4):
                        x = (shifted - 8 * m - 4 * s) & (lanes - 1)
                        odd = (x // 16) & 1 == 1
                        rel = x & 15
                        from_near = jnp.where(
                            side == 0, (rel < 4).astype(jnp.int32),
                            ((rel >= 8) & (rel < 12)).astype(jnp.int32),
                        ) == 1
                        for rg in range(2):
                            o = jnp.where(odd, mine[2 + rg], mine[rg])
                            w = jnp.where(odd, near[2 + rg], near[rg])
                            both[m, rg] = jnp.where(from_near, w, o)
                    for j in range(SLOTS):
                        x = (shifted - 8 * j - 4 * s) & (lanes - 1)
                        v = jnp.where(x >= 64, both[j % 4, 1], both[j % 4, 0])
                        e[g * SLOTS + j] = pltpu.roll(v, (lanes - 8 * j - 4 * s) % lanes, 1)
            return carry

        for i in range(groups // 2):
            unpack(i, 0)

    x_at = shifted & (lanes - 1)
    far_rows, far_layers = x_at >= 64, (x_at // 16) & 1 == 1
    top, bottom = row == 0, row == rows - 1
    across = (top & far_rows) | (bottom & ~far_rows)

    def other_half(a):
        return jnp.where(far_layers, pltpu.roll(a, 16, 1), pltpu.roll(a, lanes - 16, 1))

    def edge_factor():
        ends = factor(lambda k: elc[k], ep, eb, erl, list(range(half)), True)
        for h, (iq, beta) in enumerate(ends):
            eiq[h] = iq
            ebeta[h] = beta

    def edge_step(h):
        inv = inverse(h)

        def explicit(k, total):
            u = eu[k]
            up, down = pltpu.roll(u, 1, 0), pltpu.roll(u, rows - 1, 0)
            over = pltpu.roll(jnp.where(top, up, down), 64, 1)
            over = jnp.where(across, over, 0.0)
            up, down = jnp.where(top, over, up), jnp.where(bottom, over, down)
            beside = (up + down) + (pltpu.roll(u, 1, 1) + pltpu.roll(u, lanes - 1, 1))
            e = inv * u + epc[k] * (beside - 4.0 * u) + esrc[k]
            total = total + (ep[h, k] * erl[k]) * e
            ef[k] = total * eb[h, k]
            return total

        total = loop(n, explicit, jnp.zeros(full, jnp.float32), EXPLICIT)
        iq, beta = eiq[h], ebeta[h]
        face = total * iq
        v = meet(face, beta, iq, other_half(face), other_half(beta))

        def put(k, total):
            eu[k] = ep[h, k] * total

        suffix(ef, v, put)

    def edge_give():
        def give(g, carry):
            moved = [pltpu.roll(eu[g * SLOTS + j], 8 * j, 1) for j in range(SLOTS)]
            for q in range(4):
                b = 16 * (q // 2) + 64 * (q % 2)
                at = ((lane - b) & (lanes - 1)) // WIDTH
                ret_s[q, g] = pltpu.roll(tree(moved, at), (lanes - b) % lanes, 1)
            return carry

        for i in range(groups):
            give(i, 0)
        for s in range(2):

            @pl.when(gz == 1 - s)
            def _(s=s):
                for q in range(4):
                    if q != 2 * (1 - s) + CORE:
                        remote(
                            ret_s.at[q], ret_r.at[s], ret_ss.at[q], ret_rs.at[s],
                            (q // 2, q % 2, gy),
                        ).start()
                for g in range(groups):
                    ret_r[s, g] = ret_s[2 * (1 - s) + CORE, g]

    for a in (1, 3):
        loads[a].wait()
    for i in range(groups // 2):
        pack(i, 0)
    un.wait()
    v = vn = None
    faces = []
    tails = []
    for h in range(half):
        total = explicit_own(h, v, vn)
        face = total * iq_s[h]
        face_s[h] = face
        sends = []
        for s, peer in enumerate(peers):
            if s == 0 or h < last:
                c = remote(face_s.at[h], face_r.at[h, s], fa_ss.at[3 * h + s], fa_rs.at[3 * h + s], peer)
                c.start()
                sends.append(c)
        faces.append(sends)
        if h == 0:
            far_sends()
            own_sends()
        behind_own(h < last)
        if h < last:
            c = remote(tr_s, tr_r.at[h], tr_ss.at[h], tr_rs.at[h], x_peer)
            c.start()
            tails.append(c)
        if h == 0:
            hs = list(range(1, half))
            for i, (iq, beta) in zip(hs, factor(None, p_s, b_s, rl_s, hs, False, pr_s)):
                iq_s[i] = iq
                beta_s[i] = beta
            for i in hs:
                send_betas(i)
        if h == EDGE_AT:
            edge_wait()

            @pl.when(owner)
            def _():
                edge_unpack()
                edge_factor()
                for i in range(EDGE_SPLIT):
                    edge_step(i)

        if h == EDGE_AT:

            @pl.when(owner)
            def _():
                for i in range(EDGE_SPLIT, half):
                    edge_step(i)
                edge_give()

        for c in betas[h]:
            c.wait()
        if h < last:
            tails[h].wait()
        for c in sends:
            c.wait()
        iq, beta = iq_s[h], beta_s[h]
        v = meet(face_s[h], beta, iq, face_r[h, 0], beta_r[h, 0])
        if h < last:
            w = meet(face_r[h, 1], beta_r[h, 1], iq_r[h], face_r[h, 2], beta_r[h, 2])
            vn = jnp.where(is_low, spread(w[0:1]), spread(w[rows - 1:rows]))

    for s in range(2):

        @pl.when(me != 2 * (1 - s) + CORE)
        def _(s=s):
            remote(
                ret_s.at[0], ret_r.at[s], ret_ss.at[0], ret_rs.at[s], x_peer
            ).wait_recv()

    outer = (lane < 4) | (lane >= lanes - 4)

    def write(g, carry):
        both = jnp.where(low, ret_r[1, g], ret_r[0, g])
        for j in range(SLOTS):
            k = g * SLOTS + j
            u = p_s[last, k] * (v + t_s[k])
            out[layer(k)] = jnp.where(outer, pltpu.roll(both, (lanes - 4 - 8 * j) % lanes, 1), u)
        return carry

    for i in range(groups):
        write(i, 0)

    @pl.when(has_left)
    def _():
        to_side(0, 0).wait_send()

    @pl.when(has_right)
    def _():
        to_side(1, 0).wait_send()

    for s in range(2):

        @pl.when(me != 2 * (1 - s) + CORE)
        def _(s=s):
            to_owner(s, 0).wait_send()

    @pl.when(owner)
    def _():
        for q in range(4):

            @pl.when(me != q)
            def _(q=q):
                remote(
                    ret_s.at[q], ret_r.at[0], ret_ss.at[q], ret_rs.at[0], x_peer
                ).wait_send()


def solution(mesh):
    ny_parts = mesh.shape["gy"]
    assert mesh.shape["gz"] == 2 and mesh.shape["gx"] == 2

    def on_device(u, pc, lc, src, table, index):
        half = index.shape[0]
        n, rows, lanes = u.shape
        groups = n // SLOTS
        assert (rows, lanes, half) == (8, 128, 4) and n % (2 * SLOTS) == 0

        def vmem(*dims):
            return pltpu.VMEM(dims, jnp.float32)

        def tiles(*dims):
            return vmem(*dims, rows, lanes)

        dma = pltpu.SemaphoreType.DMA
        scratch = [tiles(n)] * 5 + [tiles(half, n)] * 2 + [tiles(n)] * 2
        scratch += [vmem(n, 1, lanes), vmem(n, 1, lanes), vmem(half - 1, n, 1, lanes)]
        scratch += [vmem(n, 1, lanes), vmem(half - 1, n, 1, lanes), vmem(half - 1, n, 1, lanes)]
        scratch += [tiles(half), tiles(half, 3), tiles(half), tiles(half - 1)]
        scratch += [tiles(half), tiles(half, 3)]
        scratch += [tiles(2, 4 * groups), tiles(2, 2 * groups), tiles(4, 4 * groups), tiles(4, 2 * groups)]
        scratch += [tiles(n)] * 5 + [tiles(half, n)] * 2 + [tiles(n)] + [tiles(half)] * 2
        scratch += [tiles(4, groups), tiles(2, groups)]
        scratch += [dma((4,)), dma((2,))]
        scratch += [dma((half - 1,))] * 4
        scratch += [dma((3 * half,))] * 2
        scratch += [dma((half - 1,))] * 2
        scratch += [dma((3 * half,))] * 2
        scratch += [pltpu.SemaphoreType.REGULAR] * 2
        scratch += [dma((2,)), dma((4,)), dma((2,)), dma((4,)), dma((4,)), dma((2,))]
        return pl.pallas_call(
            functools.partial(kernel, ny_parts, half),
            out_shape=pltpu.VMEM(u.shape, jnp.float32),
            in_specs=[pl.BlockSpec(memory_space=pl.ANY)] * 4
            + [pl.BlockSpec(memory_space=pltpu.SMEM)] * 2,
            out_specs=pl.BlockSpec(memory_space=pltpu.VMEM),
            scratch_shapes=scratch,
            compiler_params=pltpu.CompilerParams(collective_id=0, has_side_effects=True),
        )(u, pc, lc, src, table, index)

    spec = P("gz", "gx", "gy")
    return jax.shard_map(
        on_device, mesh=mesh, in_specs=(spec,) * 4 + (P(), P()), out_specs=spec, check_vma=False
    )
```
